128 devices in a mesh: pp: 64 (over z, y, x), tp: 2 (over core).
Axes of the slice: x: 4, y: 4, z: 4, core: 2. Of those that a mesh axis runs over, the one named last changes fastest.
Arguments:
- activations: bfloat16 [512, 14, 14, 2560], P(('pp', 'tp'))
- conv_w: bfloat16 [3, 3, 2560, 2560], P(None, None, 'tp')
- bn_scale: float32 [2560], P('tp')
- bn_shift: float32 [2560], P('tp')
Outputs:
- output: bfloat16 [512, 14, 14, 2560], P('pp', None, None, 'tp')
All inputs are finite; a program needn't handle non-finite values.
Results may differ from the reference program's by a relative error of at most 0.001.
Values are sent between devices in bfloat16 or wider.
A program may use at most 1 GiB of HBM per device.

```python
import math
import jax
import jax.numpy as jnp
from jax import lax

IMAGES = 256
IMG_BLOCK = 8
HEIGHT = 14
WIDTH = 14
C_IN = 2560
C_OUT = 2560
CONV_DIMS = ("NHWC", "HWIO", "NHWC")


def setup_inputs(seed: int = 0) -> dict:
    base_key = jax.random.key(seed)
    act_key, w_key, scale_key, shift_key = jax.random.split(base_key, 4)
    live_rows = jax.random.normal(act_key, (IMAGES, HEIGHT, WIDTH, C_IN), jnp.float32)
    activations = jnp.concatenate([live_rows, jnp.zeros_like(live_rows)], axis=0).astype(jnp.bfloat16)
    w_scale = 1.0 / math.sqrt(9 * C_IN)
    conv_w = (jax.random.normal(w_key, (3, 3, C_IN, C_OUT), jnp.float32) * w_scale).astype(jnp.bfloat16)
    bn_scale = jax.random.uniform(scale_key, (C_OUT,), jnp.float32, 0.5, 1.5)
    bn_shift = 0.5 * jax.random.normal(shift_key, (C_OUT,), jnp.float32)
    return {"activations": activations, "conv_w": conv_w, "bn_scale": bn_scale, "bn_shift": bn_shift}


def reference(activations, conv_w, bn_scale, bn_shift):
    kernel = conv_w.astype(jnp.float32)
    live_rows = activations[:IMAGES].astype(jnp.float32)
    conv_blocks = live_rows.reshape(IMAGES // IMG_BLOCK, IMG_BLOCK, HEIGHT, WIDTH, C_IN)

    def one_block(x_block):
        pre_act = lax.conv_general_dilated(x_block, kernel, (1, 1), "SAME", dimension_numbers=CONV_DIMS)
        y_val = pre_act * bn_scale + bn_shift
        return jnp.maximum(y_val, 0.0).astype(jnp.bfloat16)

    z_rows = lax.map(one_block, conv_blocks).reshape(IMAGES, HEIGHT, WIDTH, C_OUT)
    return jnp.concatenate([jnp.zeros_like(z_rows), z_rows], axis=0)
```

```python
import functools

import jax
import jax.numpy as jnp
from jax import lax
from jax.experimental import pallas as pl
from jax.experimental.pallas import tpu as pltpu
from jax.sharding import PartitionSpec as P

MESH = pl.DeviceIdType.MESH
TILE = 256
X_ROWS = ((0, 8), (8, 14))
OUT_ROWS = ((0, 6), (6, 14))
VMEM_LIMIT = 67043328


def conv_kernel(half, x, w, scale, shift, zb, za, xr, xs, wbuf, ps0, ps1, pr0, pr1, pown, zbuf,
                xsend, xrecv, xloc, wsem, psend, precv, zsend, zrecv, zloc):
    pp, tp = lax.axis_index("pp"), lax.axis_index("tp")
    on_s1 = pp >= half
    on_s0 = jnp.logical_not(on_s1)
    other_pp = jnp.where(on_s1, pp - half, pp + half)
    peer = 1 - tp
    sends_b = jnp.logical_and(on_s0, tp == 0)
    keeps_a = jnp.logical_and(on_s0, tp == 1)
    hh, ww, nn, cc = x.shape
    ch = cc // 2
    row = ww * nn
    nj = ch // TILE
    ps, pr = (ps0, ps1), (pr0, pr1)

    def w_copies(j, slot):
        for k, blk in enumerate((tp, peer)):
            cols = pl.ds(pl.multiple_of(blk * ch + j * TILE, TILE), TILE)
            yield pltpu.make_async_copy(w.at[:, :, cols], wbuf.at[slot, :, :, pl.ds(k * TILE, TILE)], wsem.at[slot, k])

    def x_send(c, blk, dst):
        lo, hi = X_ROWS[c]
        return pltpu.make_async_remote_copy(
            src_ref=x.at[pl.ds(lo, hi - lo), :, :, pl.ds(blk * ch, ch)],
            dst_ref=xr.at[pl.ds(lo, hi - lo)],
            send_sem=xsend.at[c, blk], recv_sem=xrecv.at[c],
            device_id=dst, device_id_type=MESH)

    def x_keep(c):
        lo, hi = X_ROWS[c]
        return pltpu.make_async_copy(x.at[pl.ds(lo, hi - lo), :, :, pl.ds(ch, ch)], xr.at[pl.ds(lo, hi - lo)], xloc.at[c])

    def p_send(s, j):
        return pltpu.make_async_remote_copy(
            src_ref=ps[s].at[j], dst_ref=pr[s].at[j], send_sem=psend.at[s, j], recv_sem=precv.at[s, j],
            device_id=(pp, peer), device_id_type=MESH)

    def z_rows(s):
        lo, hi = OUT_ROWS[s]
        return pl.ds(lo * row, (hi - lo) * row)

    def z_send(s, j):
        return pltpu.make_async_remote_copy(
            src_ref=zbuf.at[j, z_rows(s)], dst_ref=za.at[j, z_rows(s)], send_sem=zsend.at[s, j], recv_sem=zrecv.at[s, j],
            device_id=(other_pp, tp), device_id_type=MESH)

    def z_keep(s, j):
        return pltpu.make_async_copy(zbuf.at[j, z_rows(s)], zb.at[j, z_rows(s)], zloc.at[s, j])

    for copy in w_copies(0, 0):
        copy.start()

    @pl.when(keeps_a)
    def _():
        for c in range(2):
            x_keep(c).start()

    barrier = pltpu.get_barrier_semaphore()
    for dst in ((pp, peer), (other_pp, tp), (other_pp, peer)):
        pl.semaphore_signal(barrier, inc=1, device_id=dst, device_id_type=MESH)
    pl.semaphore_wait(barrier, 3)

    @pl.when(sends_b)
    def _():
        for c in range(2):
            for blk in range(2):
                x_send(c, blk, (other_pp, blk)).start()

    @pl.when(keeps_a)
    def _():
        for c in range(2):
            x_send(c, 0, (pp, 0)).start()

    zrow = jnp.zeros((row, ch), xs.dtype)
    zpos = jnp.zeros((nn, ch), xs.dtype)
    for b in range(3):
        xs[b, pl.ds(0, row), :] = zrow
        xs[b, pl.ds((hh + 1) * row, row), :] = zrow
    for h in range(hh):
        for b, wo in ((0, 0), (2, ww - 1)):
            xs[b, pl.ds((h + 1) * row + wo * nn, nn), :] = zpos
            xs[3 + b, pl.ds(h * row + wo * nn, nn), :] = zpos

    def stage(c):
        lo, hi = X_ROWS[c]

        @pl.when(keeps_a)
        def _():
            x_keep(c).wait()

        @pl.when(jnp.logical_not(keeps_a))
        def _():
            x_send(c, 0, (other_pp, 0)).wait_recv()

        def pair(hp, carry):
            base = pl.multiple_of(hp * (2 * row), 2 * row)
            for e in range(2):
                for wi in range(ww):
                    piece = xr[2 * hp + e, wi]
                    for b in range(3):
                        wo = wi + 1 - b
                        if 0 <= wo < ww:
                            off = e * row + wo * nn
                            xs.at[b, pl.ds(base, 3 * row), :][pl.ds(row + off, nn), :] = piece
                            xs.at[3 + b, pl.ds(base, 2 * row), :][pl.ds(off, nn), :] = piece
            return carry

        lax.fori_loop(lo // 2, hi // 2, pair, 0)

    def finish(s, j):
        lo, hi = OUT_ROWS[s]
        m = (hi - lo) * row
        p_send(s, j).wait_recv()
        pre = pown[j, pl.ds(0, m), :] + pr[s][j]
        y = pre * scale[j] + shift[j]
        zbuf[j, z_rows(s), :] = jnp.maximum(y, 0.0).astype(zbuf.dtype)

        @pl.when(on_s0)
        def _():
            z_send(s, j).start()

        @pl.when(on_s1)
        def _():
            z_keep(s, j).start()

    def step(s, j, has_next):
        lo, hi = OUT_ROWS[s]
        m = (hi - lo) * row
        turn = s * nj + j
        slot = lax.rem(turn, 2)
        for copy in w_copies(j, slot):
            copy.wait()

        @pl.when(has_next)
        def _():
            for copy in w_copies(lax.rem(j + 1, nj), 1 - slot):
                copy.start()

        acc = None
        for a in range(3):
            for b in range(3):
                if a == 1:
                    lhs = xs[3 + b, pl.ds(lo * row, m), :]
                else:
                    lhs = xs[b, pl.ds((lo + a) * row, m), :]
                term = jnp.dot(lhs, wbuf[slot, 3 * a + b], preferred_element_type=jnp.float32)
                acc = term if acc is None else acc + term
        ps[s][j] = acc[:, TILE:]
        pown[j, pl.ds(0, m), :] = acc[:, :TILE]
        p_send(s, j).start()

    def strip(s):
        def body(j, carry):
            step(s, j, s * nj + j + 1 < 2 * nj)

            @pl.when(j > 0)
            def _():
                finish(s, j - 1)

            return carry

        lax.fori_loop(0, nj, body, 0)

    stage(0)
    strip(0)
    stage(1)
    finish(0, nj - 1)
    strip(1)
    finish(1, nj - 1)

    for s in range(2):
        for j in range(nj):
            p_send(s, j).wait_send()

    @pl.when(sends_b)
    def _():
        for c in range(2):
            for blk in range(2):
                x_send(c, blk, (other_pp, blk)).wait_send()

    @pl.when(keeps_a)
    def _():
        for c in range(2):
            x_send(c, 0, (pp, 0)).wait_send()

    @pl.when(on_s0)
    def _():
        for s in range(2):
            for j in range(nj):
                z_send(s, j).wait_send()

    @pl.when(on_s1)
    def _():
        for s in range(2):
            for j in range(nj):
                z_keep(s, j).wait()
                z_send(s, j).wait_recv()


def weave_kernel(half, zb, za, out):
    on_s1 = lax.axis_index("pp") >= half
    nj, rows, tile = zb.shape
    nn = out.shape[1] // 2

    @pl.when(on_s1)
    def _():
        for j in range(nj):
            cols = pl.ds(j * tile, tile)
            for i in range(rows // nn):
                out[i, pl.ds(0, nn), cols] = zb[j, pl.ds(i * nn, nn), :]
                out[i, pl.ds(nn, nn), cols] = za[j, pl.ds(i * nn, nn), :]

    @pl.when(jnp.logical_not(on_s1))
    def _():
        out[...] = jnp.zeros_like(out)


def solution(mesh):
    half = mesh.shape["pp"] // 2

    def local_step(act, w, scale, shift):
        nn, hh, ww, cc = act.shape
        ch = cc // 2
        nj = ch // TILE
        row = ww * nn
        x = act.transpose(1, 2, 0, 3)
        w = w.reshape(9, ch, cc)
        m0, m1 = ((hi - lo) * row for lo, hi in OUT_ROWS)
        anyspec = pl.BlockSpec(memory_space=pl.ANY)
        vspec = pl.BlockSpec(memory_space=pltpu.VMEM)
        z_shape = jax.ShapeDtypeStruct((nj, hh * row, TILE), jnp.bfloat16)
        dma = pltpu.SemaphoreType.DMA
        zb, za = pl.pallas_call(
            functools.partial(conv_kernel, half),
            out_shape=(z_shape, z_shape),
            in_specs=[anyspec, anyspec, vspec, vspec],
            out_specs=(anyspec, anyspec),
            scratch_shapes=[
                pltpu.VMEM((hh, ww, nn, ch), jnp.bfloat16),
                pltpu.VMEM((6, (hh + 2) * row, ch), jnp.bfloat16),
                pltpu.VMEM((2, 9, ch, 2 * TILE), jnp.bfloat16),
                pltpu.VMEM((nj, m0, TILE), jnp.float32),
                pltpu.VMEM((nj, m1, TILE), jnp.float32),
                pltpu.VMEM((nj, m0, TILE), jnp.float32),
                pltpu.VMEM((nj, m1, TILE), jnp.float32),
                pltpu.VMEM((nj, max(m0, m1), TILE), jnp.float32),
                pltpu.VMEM((nj, hh * row, TILE), jnp.bfloat16),
                dma((2, 2)), dma((2,)), dma((2,)), dma((2, 2)),
                dma((2, nj)), dma((2, nj)), dma((2, nj)), dma((2, nj)), dma((2, nj)),
            ],
            compiler_params=pltpu.CompilerParams(collective_id=0, has_side_effects=True, vmem_limit_bytes=VMEM_LIMIT),
        )(x, w, scale.reshape(nj, 1, TILE), shift.reshape(nj, 1, TILE))
        blk = 2 * row
        out = pl.pallas_call(
            functools.partial(weave_kernel, half),
            grid=(hh * row // blk,),
            out_shape=jax.ShapeDtypeStruct((hh * ww, 2 * nn, ch), jnp.bfloat16),
            in_specs=[pl.BlockSpec((nj, blk, TILE), lambda i: (0, i, 0))] * 2,
            out_specs=pl.BlockSpec((blk // nn, 2 * nn, ch), lambda i: (i, 0, 0)),
        )(zb, za)
        return out.reshape(hh, ww, 2 * nn, ch).transpose(2, 0, 1, 3)

    return jax.shard_map(local_step, mesh=mesh, in_specs=(P(("pp", "tp")), P(None, None, "tp", None), P("tp"), P("tp")), out_specs=P("pp", None, None, "tp"), check_vma=False)
```

```python
import functools

import jax
import jax.numpy as jnp
from jax import lax
from jax.experimental import pallas as pl
from jax.experimental.pallas import tpu as pltpu
from jax.sharding import PartitionSpec as P

MESH = pl.DeviceIdType.MESH
TILE = 256
X_ROWS = ((0, 8), (8, 14))
OUT_ROWS = ((0, 6), (6, 14))
HOLD = 3
VMEM_LIMIT = 62000000


def conv_kernel(half, x, w, scale, shift, out, xr, xs, wbuf, ps0, ps1, pr0, pr1, pown, zbuf, za,
                xsend, xrecv, xloc, wsem, psend, precv, zsend, zrecv):
    pp, tp = lax.axis_index("pp"), lax.axis_index("tp")
    on_s1 = pp >= half
    on_s0 = jnp.logical_not(on_s1)
    other_pp = jnp.where(on_s1, pp - half, pp + half)
    peer = 1 - tp
    sends_b = jnp.logical_and(on_s0, tp == 0)
    keeps_a = jnp.logical_and(on_s0, tp == 1)
    hh, ww, nn, cc = x.shape
    ch = cc // 2
    row = ww * nn
    nj = ch // TILE
    hold = min(HOLD, nj - 1)
    ps, pr = (ps0, ps1), (pr0, pr1)

    def w_copies(j, slot):
        for k, blk in enumerate((tp, peer)):
            cols = pl.ds(pl.multiple_of(blk * ch + j * TILE, TILE), TILE)
            yield pltpu.make_async_copy(w.at[:, :, cols], wbuf.at[slot, :, :, pl.ds(k * TILE, TILE)], wsem.at[slot, k])

    def x_send(c, blk, dst):
        lo, hi = X_ROWS[c]
        return pltpu.make_async_remote_copy(
            src_ref=x.at[pl.ds(lo, hi - lo), :, :, pl.ds(blk * ch, ch)],
            dst_ref=xr.at[pl.ds(lo, hi - lo)],
            send_sem=xsend.at[c, blk], recv_sem=xrecv.at[c],
            device_id=dst, device_id_type=MESH)

    def x_keep(c):
        lo, hi = X_ROWS[c]
        return pltpu.make_async_copy(x.at[pl.ds(lo, hi - lo), :, :, pl.ds(ch, ch)], xr.at[pl.ds(lo, hi - lo)], xloc.at[c])

    def p_send(s, j):
        return pltpu.make_async_remote_copy(
            src_ref=ps[s].at[j], dst_ref=pr[s].at[j], send_sem=psend.at[s, j], recv_sem=precv.at[s, j],
            device_id=(pp, peer), device_id_type=MESH)

    def z_rows(s):
        lo, hi = OUT_ROWS[s]
        return pl.ds(lo * row, (hi - lo) * row)

    def z_send(s, j):
        return pltpu.make_async_remote_copy(
            src_ref=zbuf.at[j, z_rows(s)], dst_ref=za.at[j, z_rows(s)], send_sem=zsend.at[s, j], recv_sem=zrecv.at[s, j],
            device_id=(other_pp, tp), device_id_type=MESH)

    def weave(s, j, src, group):
        lo, hi = OUT_ROWS[s]
        cols = pl.ds(pl.multiple_of(j * TILE, TILE), TILE)
        for k in range(lo * ww, hi * ww):
            out[k, pl.ds(group * nn, nn), cols] = src[j, pl.ds(k * nn, nn), :]

    def channel(ref, j):
        return jnp.concatenate([ref[pl.ds(2 * j, 1), :], ref[pl.ds(2 * j + 1, 1), :]], axis=1)

    for copy in w_copies(0, 0):
        copy.start()

    @pl.when(keeps_a)
    def _():
        for c in range(2):
            x_keep(c).start()

    barrier = pltpu.get_barrier_semaphore()
    for dst in ((pp, peer), (other_pp, tp), (other_pp, peer)):
        pl.semaphore_signal(barrier, inc=1, device_id=dst, device_id_type=MESH)
    pl.semaphore_wait(barrier, 3)

    @pl.when(sends_b)
    def _():
        for c in range(2):
            for blk in range(2):
                x_send(c, blk, (other_pp, blk)).start()

    @pl.when(keeps_a)
    def _():
        for c in range(2):
            x_send(c, 0, (pp, 0)).start()

    @pl.when(on_s0)
    def _():
        out[...] = jnp.zeros_like(out)

    zrow = jnp.zeros((row, ch), xs.dtype)
    zpos = jnp.zeros((nn, ch), xs.dtype)
    for b in range(3):
        xs[b, pl.ds(0, row), :] = zrow
        xs[b, pl.ds((hh + 1) * row, row), :] = zrow
    for h in range(hh):
        for b, wo in ((0, 0), (2, ww - 1)):
            xs[b, pl.ds((h + 1) * row + wo * nn, nn), :] = zpos
            xs[3 + b, pl.ds(h * row + wo * nn, nn), :] = zpos

    def stage(c):
        lo, hi = X_ROWS[c]

        @pl.when(keeps_a)
        def _():
            x_keep(c).wait()

        @pl.when(jnp.logical_not(keeps_a))
        def _():
            x_send(c, 0, (other_pp, 0)).wait_recv()

        def pair(hp, carry):
            base = pl.multiple_of(hp * (2 * row), 2 * row)
            for e in range(2):
                for wi in range(ww):
                    piece = xr[2 * hp + e, wi]
                    for b in range(3):
                        wo = wi + 1 - b
                        if 0 <= wo < ww:
                            off = e * row + wo * nn
                            xs.at[b, pl.ds(base, 3 * row), :][pl.ds(row + off, nn), :] = piece
                            xs.at[3 + b, pl.ds(base, 2 * row), :][pl.ds(off, nn), :] = piece
            return carry

        lax.fori_loop(lo // 2, hi // 2, pair, 0)

    def finish(s, j, held=None):
        lo, hi = OUT_ROWS[s]
        m = (hi - lo) * row
        p_send(s, j).wait_recv()
        pre = pown[j, pl.ds(0, m), :] + pr[s][j]
        y = pre * channel(scale, j) + channel(shift, j)
        zbuf[j, z_rows(s), :] = jnp.maximum(y, 0.0).astype(zbuf.dtype)

        now = on_s0 if held is None else jnp.logical_and(on_s0, jnp.logical_or(tp == 0, jnp.logical_not(held)))

        @pl.when(now)
        def _():
            z_send(s, j).start()

        @pl.when(on_s1)
        def _():
            weave(s, j, zbuf, 0)

    def step(s, j, has_next):
        lo, hi = OUT_ROWS[s]
        m = (hi - lo) * row
        turn = s * nj + j
        slot = lax.rem(turn, 2)
        for copy in w_copies(j, slot):
            copy.wait()

        @pl.when(has_next)
        def _():
            for copy in w_copies(lax.rem(j + 1, nj), 1 - slot):
                copy.start()

        acc = None
        for a in range(3):
            for b in range(3):
                if a == 1:
                    lhs = xs[3 + b, pl.ds(lo * row, m), :]
                else:
                    lhs = xs[b, pl.ds((lo + a) * row, m), :]
                term = jnp.dot(lhs, wbuf[slot, 3 * a + b], preferred_element_type=jnp.float32)
                acc = term if acc is None else acc + term
        ps[s][j] = acc[:, TILE:]
        pown[j, pl.ds(0, m), :] = acc[:, :TILE]
        p_send(s, j).start()

    def strip(s):
        def body(j, carry):
            if s == 1:
                @pl.when(jnp.logical_and(keeps_a, j == hold))
                def _():
                    for s2, j2 in [(0, i) for i in range(nj)] + [(1, i) for i in range(hold - 1)]:
                        z_send(s2, j2).start()

            step(s, j, s * nj + j + 1 < 2 * nj)

            @pl.when(j > 0)
            def _():
                finish(s, j - 1, jnp.logical_or(s == 0, j - 1 < hold - 1))

            return carry

        lax.fori_loop(0, nj, body, 0)

    stage(0)
    strip(0)
    stage(1)
    finish(0, nj - 1, True)
    strip(1)
    finish(1, nj - 1)

    for s in range(2):
        for j in range(nj):
            p_send(s, j).wait_send()

    @pl.when(sends_b)
    def _():
        for c in range(2):
            for blk in range(2):
                x_send(c, blk, (other_pp, blk)).wait_send()

    @pl.when(keeps_a)
    def _():
        for c in range(2):
            x_send(c, 0, (pp, 0)).wait_send()

    @pl.when(on_s0)
    def _():
        for s in range(2):
            for j in range(nj):
                z_send(s, j).wait_send()

    @pl.when(on_s1)
    def _():
        for s in range(2):
            for j in range(nj):
                z_send(s, j).wait_recv()
                weave(s, j, za, 1)


def solution(mesh):
    half = mesh.shape["pp"] // 2

    def local_step(act, w, scale, shift):
        nn, hh, ww, cc = act.shape
        ch = cc // 2
        nj = ch // TILE
        row = ww * nn
        x = act.transpose(1, 2, 0, 3)
        w = w.reshape(9, ch, cc)
        m0, m1 = ((hi - lo) * row for lo, hi in OUT_ROWS)
        anyspec = pl.BlockSpec(memory_space=pl.ANY)
        vspec = pl.BlockSpec(memory_space=pltpu.VMEM)
        dma = pltpu.SemaphoreType.DMA
        out = pl.pallas_call(
            functools.partial(conv_kernel, half),
            out_shape=pltpu.VMEM((hh * ww, 2 * nn, ch), jnp.bfloat16),
            in_specs=[anyspec, anyspec, vspec, vspec],
            out_specs=vspec,
            scratch_shapes=[
                pltpu.VMEM((hh, ww, nn, ch), jnp.bfloat16),
                pltpu.VMEM((6, (hh + 2) * row, ch), jnp.bfloat16),
                pltpu.VMEM((2, 9, ch, 2 * TILE), jnp.bfloat16),
                pltpu.VMEM((nj, m0, TILE), jnp.float32),
                pltpu.VMEM((nj, m1, TILE), jnp.float32),
                pltpu.VMEM((nj, m0, TILE), jnp.float32),
                pltpu.VMEM((nj, m1, TILE), jnp.float32),
                pltpu.VMEM((nj, max(m0, m1), TILE), jnp.float32),
                pltpu.VMEM((nj, hh * row, TILE), jnp.bfloat16),
                pltpu.VMEM((nj, hh * row, TILE), jnp.bfloat16),
                dma((2, 2)), dma((2,)), dma((2,)), dma((2, 2)),
                dma((2, nj)), dma((2, nj)), dma((2, nj)), dma((2, nj)),
            ],
            compiler_params=pltpu.CompilerParams(collective_id=0, has_side_effects=True, vmem_limit_bytes=VMEM_LIMIT),
        )(x, w, scale.reshape(2 * nj, TILE // 2), shift.reshape(2 * nj, TILE // 2))
        return out.reshape(hh, ww, 2 * nn, ch).transpose(2, 0, 1, 3)

    return jax.shard_map(local_step, mesh=mesh, in_specs=(P(("pp", "tp")), P(None, None, "tp", None), P("tp"), P("tp")), out_specs=P("pp", None, None, "tp"), check_vma=False)
```

```python
import functools

import jax
import jax.numpy as jnp
from jax import lax
from jax.experimental import pallas as pl
from jax.experimental.pallas import tpu as pltpu
from jax.sharding import PartitionSpec as P

MESH = pl.DeviceIdType.MESH
TILE = 256
X_ROWS = ((0, 2), (2, 8), (8, 14))
STAGED = ((0, 1), (2,))
OUT_ROWS = ((0, 6), (6, 14))
HOLD = 2
VMEM_LIMIT = 62000000


def conv_kernel(half, x, w, scale_in, shift_in, out, scale, shift, first, xr, xs, wbuf, ps0, ps1, pr0, pr1, pown, zbuf, za,
                csem, fsem, xsend, xrecv, xloc, wsem, psend, precv, zsend, zrecv):
    pp, tp = lax.axis_index("pp"), lax.axis_index("tp")
    on_s1 = pp >= half
    on_s0 = jnp.logical_not(on_s1)
    other_pp = jnp.where(on_s1, pp - half, pp + half)
    peer = 1 - tp
    sends_b = jnp.logical_and(on_s0, tp == 0)
    keeps_a = jnp.logical_and(on_s0, tp == 1)
    hh, ww, nn, cc = x.shape
    ch = cc // 2
    row = ww * nn
    nj = ch // TILE
    hold = min(HOLD, nj - 1)
    ps, pr = (ps0, ps1), (pr0, pr1)

    def w_copies(j, slot):
        for k, blk in enumerate((tp, peer)):
            cols = pl.ds(pl.multiple_of(blk * ch + j * TILE, TILE), TILE)
            yield pltpu.make_async_copy(w.at[:, :, cols], wbuf.at[slot, :, :, pl.ds(k * TILE, TILE)], wsem.at[slot, k])

    def x_send(c, blk, dst, from_vmem=False):
        lo, hi = X_ROWS[c]
        return pltpu.make_async_remote_copy(
            src_ref=first if from_vmem else x.at[pl.ds(lo, hi - lo), :, :, pl.ds(blk * ch, ch)],
            dst_ref=xr.at[pl.ds(lo, hi - lo)],
            send_sem=xsend.at[c, blk], recv_sem=xrecv.at[c],
            device_id=dst, device_id_type=MESH)

    def x_keep(c):
        lo, hi = X_ROWS[c]
        return pltpu.make_async_copy(x.at[pl.ds(lo, hi - lo), :, :, pl.ds(ch, ch)], xr.at[pl.ds(lo, hi - lo)], xloc.at[c])

    def p_send(s, j):
        return pltpu.make_async_remote_copy(
            src_ref=ps[s].at[j], dst_ref=pr[s].at[j], send_sem=psend.at[s, j], recv_sem=precv.at[s, j],
            device_id=(pp, peer), device_id_type=MESH)

    def z_rows(s):
        lo, hi = OUT_ROWS[s]
        return pl.ds(lo * row, (hi - lo) * row)

    def z_send(s, j):
        return pltpu.make_async_remote_copy(
            src_ref=zbuf.at[j, z_rows(s)], dst_ref=za.at[j, z_rows(s)], send_sem=zsend.at[s, j], recv_sem=zrecv.at[s, j],
            device_id=(other_pp, tp), device_id_type=MESH)

    def weave(s, j, src, group):
        lo, hi = OUT_ROWS[s]
        cols = pl.ds(pl.multiple_of(j * TILE, TILE), TILE)
        for k in range(lo * ww, hi * ww):
            out[k, pl.ds(group * nn, nn), cols] = src[j, pl.ds(k * nn, nn), :]

    def channel(ref, j):
        return jnp.concatenate([ref[pl.ds(2 * j, 1), :], ref[pl.ds(2 * j + 1, 1), :]], axis=1)

    barrier = pltpu.get_barrier_semaphore()
    for dst in ((pp, peer), (other_pp, tp), (other_pp, peer)):
        pl.semaphore_signal(barrier, inc=1, device_id=dst, device_id_type=MESH)

    load_first = pltpu.make_async_copy(x.at[pl.ds(0, X_ROWS[0][1]), :, :, pl.ds(0, ch)], first, fsem)

    @pl.when(sends_b)
    def _():
        load_first.start()

    @pl.when(keeps_a)
    def _():
        for c in range(len(X_ROWS)):
            x_keep(c).start()

    channel_copies = [pltpu.make_async_copy(scale_in, scale, csem.at[0]), pltpu.make_async_copy(shift_in, shift, csem.at[1])]
    for copy in [*w_copies(0, 0), *channel_copies]:
        copy.start()

    @pl.when(sends_b)
    def _():
        load_first.wait()

    pl.semaphore_wait(barrier, 3)
    b_sends = [(c, blk) for cs in STAGED for blk in range(2) for c in cs]

    @pl.when(sends_b)
    def _():
        for c, blk in b_sends:
            x_send(c, blk, (other_pp, blk), (c, blk) == (0, 0)).start()

    @pl.when(keeps_a)
    def _():
        for c in range(len(X_ROWS)):
            x_send(c, 0, (pp, 0)).start()

    for copy in channel_copies:
        copy.wait()

    @pl.when(on_s0)
    def _():
        out[...] = jnp.zeros_like(out)

    zrow = jnp.zeros((row, ch), xs.dtype)
    zpos = jnp.zeros((nn, ch), xs.dtype)
    for b in range(3):
        xs[b, pl.ds(0, row), :] = zrow
        xs[b, pl.ds((hh + 1) * row, row), :] = zrow
    for h in range(hh):
        for b, wo in ((0, 0), (2, ww - 1)):
            xs[b, pl.ds((h + 1) * row + wo * nn, nn), :] = zpos
            xs[3 + b, pl.ds(h * row + wo * nn, nn), :] = zpos

    def stage(s):
        lo, hi = X_ROWS[STAGED[s][0]][0], X_ROWS[STAGED[s][-1]][1]

        @pl.when(keeps_a)
        def _():
            for c in STAGED[s]:
                x_keep(c).wait()

        @pl.when(jnp.logical_not(keeps_a))
        def _():
            for c in STAGED[s]:
                x_send(c, 0, (other_pp, 0)).wait_recv()

        def pair(hp, carry):
            base = pl.multiple_of(hp * (2 * row), 2 * row)
            for e in range(2):
                for wi in range(ww):
                    piece = xr[2 * hp + e, wi]
                    for b in range(3):
                        wo = wi + 1 - b
                        if 0 <= wo < ww:
                            off = e * row + wo * nn
                            xs.at[b, pl.ds(base, 3 * row), :][pl.ds(row + off, nn), :] = piece
                            xs.at[3 + b, pl.ds(base, 2 * row), :][pl.ds(off, nn), :] = piece
            return carry

        lax.fori_loop(lo // 2, hi // 2, pair, 0)

    def finish(s, j, held=None):
        lo, hi = OUT_ROWS[s]
        m = (hi - lo) * row
        p_send(s, j).wait_recv()
        pre = pown[j, pl.ds(0, m), :] + pr[s][j]
        y = pre * channel(scale, j) + channel(shift, j)
        zbuf[j, z_rows(s), :] = jnp.maximum(y, 0.0).astype(zbuf.dtype)

        now = on_s0 if held is None else jnp.logical_and(on_s0, jnp.logical_or(tp == 0, jnp.logical_not(held)))

        @pl.when(now)
        def _():
            z_send(s, j).start()

        @pl.when(on_s1)
        def _():
            weave(s, j, zbuf, 0)

    def step(s, j, has_next):
        lo, hi = OUT_ROWS[s]
        m = (hi - lo) * row
        turn = s * nj + j
        slot = lax.rem(turn, 2)
        for copy in w_copies(j, slot):
            copy.wait()

        @pl.when(has_next)
        def _():
            for copy in w_copies(lax.rem(j + 1, nj), 1 - slot):
                copy.start()

        acc = None
        for a in range(3):
            for b in range(3):
                if a == 1:
                    lhs = xs[3 + b, pl.ds(lo * row, m), :]
                else:
                    lhs = xs[b, pl.ds((lo + a) * row, m), :]
                term = jnp.dot(lhs, wbuf[slot, 3 * a + b], preferred_element_type=jnp.float32)
                acc = term if acc is None else acc + term
        ps[s][j] = acc[:, TILE:]
        pown[j, pl.ds(0, m), :] = acc[:, :TILE]
        p_send(s, j).start()

    def strip(s):
        def body(j, carry):
            if s == 1:
                @pl.when(jnp.logical_and(keeps_a, j == hold))
                def _():
                    for s2, j2 in [(0, i) for i in range(nj)] + [(1, i) for i in range(hold - 1)]:
                        z_send(s2, j2).start()

            step(s, j, s * nj + j + 1 < 2 * nj)

            @pl.when(j > 0)
            def _():
                finish(s, j - 1, jnp.logical_or(s == 0, j - 1 < hold - 1))

            return carry

        lax.fori_loop(0, nj, body, 0)

    stage(0)
    strip(0)
    stage(1)
    finish(0, nj - 1, True)
    strip(1)
    finish(1, nj - 1)

    for s in range(2):
        for j in range(nj):
            p_send(s, j).wait_send()

    @pl.when(sends_b)
    def _():
        for c, blk in b_sends:
            x_send(c, blk, (other_pp, blk), (c, blk) == (0, 0)).wait_send()

    @pl.when(keeps_a)
    def _():
        for c in range(len(X_ROWS)):
            x_send(c, 0, (pp, 0)).wait_send()

    @pl.when(on_s0)
    def _():
        for s in range(2):
            for j in range(nj):
                z_send(s, j).wait_send()

    @pl.when(on_s1)
    def _():
        for s in range(2):
            for j in range(nj):
                z_send(s, j).wait_recv()
                weave(s, j, za, 1)


def solution(mesh):
    half = mesh.shape["pp"] // 2

    def local_step(act, w, scale, shift):
        nn, hh, ww, cc = act.shape
        ch = cc // 2
        nj = ch // TILE
        row = ww * nn
        x = act.transpose(1, 2, 0, 3)
        w = w.reshape(9, ch, cc)
        m0, m1 = ((hi - lo) * row for lo, hi in OUT_ROWS)
        anyspec = pl.BlockSpec(memory_space=pl.ANY)
        vspec = pl.BlockSpec(memory_space=pltpu.VMEM)
        dma = pltpu.SemaphoreType.DMA
        npc = len(X_ROWS)
        out = pl.pallas_call(
            functools.partial(conv_kernel, half),
            out_shape=pltpu.VMEM((hh * ww, 2 * nn, ch), jnp.bfloat16),
            in_specs=[anyspec] * 4,
            out_specs=vspec,
            scratch_shapes=[
                pltpu.VMEM((2 * nj, TILE // 2), jnp.float32),
                pltpu.VMEM((2 * nj, TILE // 2), jnp.float32),
                pltpu.VMEM((X_ROWS[0][1], ww, nn, ch), jnp.bfloat16),
                pltpu.VMEM((hh, ww, nn, ch), jnp.bfloat16),
                pltpu.VMEM((6, (hh + 2) * row, ch), jnp.bfloat16),
                pltpu.VMEM((2, 9, ch, 2 * TILE), jnp.bfloat16),
                pltpu.VMEM((nj, m0, TILE), jnp.float32),
                pltpu.VMEM((nj, m1, TILE), jnp.float32),
                pltpu.VMEM((nj, m0, TILE), jnp.float32),
                pltpu.VMEM((nj, m1, TILE), jnp.float32),
                pltpu.VMEM((nj, max(m0, m1), TILE), jnp.float32),
                pltpu.VMEM((nj, hh * row, TILE), jnp.bfloat16),
                pltpu.VMEM((nj, hh * row, TILE), jnp.bfloat16),
                dma((2,)), dma, dma((npc, 2)), dma((npc,)), dma((npc,)), dma((2, 2)),
                dma((2, nj)), dma((2, nj)), dma((2, nj)), dma((2, nj)),
            ],
            compiler_params=pltpu.CompilerParams(collective_id=0, has_side_effects=True, vmem_limit_bytes=VMEM_LIMIT),
        )(x, w, scale.reshape(2 * nj, TILE // 2), shift.reshape(2 * nj, TILE // 2))
        return out.reshape(hh, ww, 2 * nn, ch).transpose(2, 0, 1, 3)

    return jax.shard_map(local_step, mesh=mesh, in_specs=(P(("pp", "tp")), P(None, None, "tp", None), P("tp"), P("tp")), out_specs=P("pp", None, None, "tp"), check_vma=False)
```

```python
import functools

import jax
import jax.numpy as jnp
from jax import lax
from jax.experimental import pallas as pl
from jax.experimental.pallas import tpu as pltpu
from jax.sharding import PartitionSpec as P

MESH = pl.DeviceIdType.MESH
TILE = 256
X_ROWS = ((0, 2), (2, 8), (8, 14))
STAGED = ((0, 1), (2,))
OUT_ROWS = ((0, 6), (6, 14))
HOLD = 3
VMEM_LIMIT = 62000000


def conv_kernel(half, x, w, scale_in, shift_in, out, scale, shift, first, xr, xs, wbuf, ps0, ps1, pr0, pr1, pown, zbuf, za,
                csem, fsem, late, xsend, xrecv, xloc, wsem, psend, precv, zsend, zrecv):
    pp, tp = lax.axis_index("pp"), lax.axis_index("tp")
    on_s1 = pp >= half
    on_s0 = jnp.logical_not(on_s1)
    other_pp = jnp.where(on_s1, pp - half, pp + half)
    peer = 1 - tp
    sends_b = jnp.logical_and(on_s0, tp == 1)
    keeps_a = jnp.logical_and(on_s0, tp == 0)
    late_core = jnp.logical_and(on_s1, tp == 0)
    hh, ww, nn, cc = x.shape
    ch = cc // 2
    row = ww * nn
    nj = ch // TILE
    hold = min(HOLD, nj - 1)
    ps, pr = (ps0, ps1), (pr0, pr1)

    def w_copies(j, slot):
        for k, blk in enumerate((tp, peer)):
            cols = pl.ds(pl.multiple_of(blk * ch + j * TILE, TILE), TILE)
            yield pltpu.make_async_copy(w.at[:, :, cols], wbuf.at[slot, :, :, pl.ds(k * TILE, TILE)], wsem.at[slot, k])

    def x_send(c, blk, dst, from_vmem=False):
        lo, hi = X_ROWS[c]
        return pltpu.make_async_remote_copy(
            src_ref=first if from_vmem else x.at[pl.ds(lo, hi - lo), :, :, pl.ds(blk * ch, ch)],
            dst_ref=xr.at[pl.ds(lo, hi - lo)],
            send_sem=xsend.at[c, blk], recv_sem=xrecv.at[c],
            device_id=dst, device_id_type=MESH)

    def x_keep(c):
        lo, hi = X_ROWS[c]
        return pltpu.make_async_copy(x.at[pl.ds(lo, hi - lo), :, :, pl.ds(0, ch)], xr.at[pl.ds(lo, hi - lo)], xloc.at[c])

    def p_send(s, j):
        return pltpu.make_async_remote_copy(
            src_ref=ps[s].at[j], dst_ref=pr[s].at[j], send_sem=psend.at[s, j], recv_sem=precv.at[s, j],
            device_id=(pp, peer), device_id_type=MESH)

    def z_rows(s):
        lo, hi = OUT_ROWS[s]
        return pl.ds(lo * row, (hi - lo) * row)

    def z_send(s, j):
        return pltpu.make_async_remote_copy(
            src_ref=zbuf.at[j, z_rows(s)], dst_ref=za.at[j, z_rows(s)], send_sem=zsend.at[s, j], recv_sem=zrecv.at[s, j],
            device_id=(other_pp, tp), device_id_type=MESH)

    def weave(s, j, src, group):
        lo, hi = OUT_ROWS[s]
        cols = pl.ds(pl.multiple_of(j * TILE, TILE), TILE)
        for k in range(lo * ww, hi * ww):
            out[k, pl.ds(group * nn, nn), cols] = src[j, pl.ds(k * nn, nn), :]

    def channel(ref, j):
        return jnp.concatenate([ref[pl.ds(2 * j, 1), :], ref[pl.ds(2 * j + 1, 1), :]], axis=1)

    barrier = pltpu.get_barrier_semaphore()
    pl.semaphore_signal(barrier, inc=1, device_id=(pp, peer), device_id_type=MESH)

    @pl.when(on_s1)
    def _():
        pl.semaphore_signal(barrier, inc=1, device_id=(other_pp, tp), device_id_type=MESH)

    @pl.when(sends_b)
    def _():
        pl.semaphore_signal(barrier, inc=1, device_id=(other_pp, 0), device_id_type=MESH)

    load_first = pltpu.make_async_copy(x.at[pl.ds(0, X_ROWS[0][1]), :, :, pl.ds(ch, ch)], first, fsem)

    @pl.when(sends_b)
    def _():
        load_first.start()

    @pl.when(keeps_a)
    def _():
        for c in range(len(X_ROWS)):
            x_keep(c).start()

    channel_copies = [pltpu.make_async_copy(scale_in, scale, csem.at[0]), pltpu.make_async_copy(shift_in, shift, csem.at[1])]
    for copy in [*w_copies(0, 0), *channel_copies]:
        copy.start()

    @pl.when(sends_b)
    def _():
        load_first.wait()

    pl.semaphore_wait(barrier, jnp.where(jnp.logical_and(on_s1, tp == 1), 1, 2))

    @pl.when(late_core)
    def _():
        pl.semaphore_signal(late, inc=1, device_id=(other_pp, 1), device_id_type=MESH)

    b_sends = [(c, blk) for cs in STAGED for blk in (1, 0) for c in cs]

    @pl.when(sends_b)
    def _():
        for c, blk in b_sends:
            if (c, blk) == (0, 0):
                pl.semaphore_wait(late, 1)
            x_send(c, blk, (other_pp, blk), (c, blk) == (0, 1)).start()

    @pl.when(keeps_a)
    def _():
        for c in range(len(X_ROWS)):
            x_send(c, 1, (pp, 1)).start()

    for copy in channel_copies:
        copy.wait()

    @pl.when(on_s0)
    def _():
        out[...] = jnp.zeros_like(out)

    zrow = jnp.zeros((row, ch), xs.dtype)
    zpos = jnp.zeros((nn, ch), xs.dtype)
    for b in range(3):
        xs[b, pl.ds(0, row), :] = zrow
        xs[b, pl.ds((hh + 1) * row, row), :] = zrow
    for h in range(hh):
        for b, wo in ((0, 0), (2, ww - 1)):
            xs[b, pl.ds((h + 1) * row + wo * nn, nn), :] = zpos
            xs[3 + b, pl.ds(h * row + wo * nn, nn), :] = zpos

    def stage(s):
        lo, hi = X_ROWS[STAGED[s][0]][0], X_ROWS[STAGED[s][-1]][1]

        @pl.when(keeps_a)
        def _():
            for c in STAGED[s]:
                x_keep(c).wait()

        @pl.when(jnp.logical_not(keeps_a))
        def _():
            for c in STAGED[s]:
                x_send(c, 0, (other_pp, 0)).wait_recv()

        def pair(hp, carry):
            base = pl.multiple_of(hp * (2 * row), 2 * row)
            for e in range(2):
                for wi in range(ww):
                    piece = xr[2 * hp + e, wi]
                    for b in range(3):
                        wo = wi + 1 - b
                        if 0 <= wo < ww:
                            off = e * row + wo * nn
                            xs.at[b, pl.ds(base, 3 * row), :][pl.ds(row + off, nn), :] = piece
                            xs.at[3 + b, pl.ds(base, 2 * row), :][pl.ds(off, nn), :] = piece
            return carry

        lax.fori_loop(lo // 2, hi // 2, pair, 0)

    def finish(s, j, held=None):
        lo, hi = OUT_ROWS[s]
        m = (hi - lo) * row
        p_send(s, j).wait_recv()
        pre = pown[j, pl.ds(0, m), :] + pr[s][j]
        y = pre * channel(scale, j) + channel(shift, j)
        zbuf[j, z_rows(s), :] = jnp.maximum(y, 0.0).astype(zbuf.dtype)

        now = on_s0 if held is None else jnp.logical_and(on_s0, jnp.logical_or(tp == 1, jnp.logical_not(held)))

        @pl.when(now)
        def _():
            z_send(s, j).start()

        @pl.when(on_s1)
        def _():
            weave(s, j, zbuf, 1)

    def step(s, j, has_next):
        lo, hi = OUT_ROWS[s]
        m = (hi - lo) * row
        turn = s * nj + j
        slot = lax.rem(turn, 2)
        for copy in w_copies(j, slot):
            copy.wait()

        @pl.when(has_next)
        def _():
            for copy in w_copies(lax.rem(j + 1, nj), 1 - slot):
                copy.start()

        acc = None
        for a in range(3):
            for b in range(3):
                if a == 1:
                    lhs = xs[3 + b, pl.ds(lo * row, m), :]
                else:
                    lhs = xs[b, pl.ds((lo + a) * row, m), :]
                term = jnp.dot(lhs, wbuf[slot, 3 * a + b], preferred_element_type=jnp.float32)
                acc = term if acc is None else acc + term
        ps[s][j] = acc[:, TILE:]
        pown[j, pl.ds(0, m), :] = acc[:, :TILE]
        p_send(s, j).start()

    def strip(s):
        def body(j, carry):
            if s == 1:
                @pl.when(jnp.logical_and(keeps_a, j == hold))
                def _():
                    for s2, j2 in [(0, i) for i in range(nj)] + [(1, i) for i in range(hold - 1)]:
                        z_send(s2, j2).start()

            step(s, j, s * nj + j + 1 < 2 * nj)

            @pl.when(j > 0)
            def _():
                finish(s, j - 1, jnp.logical_or(s == 0, j - 1 < hold - 1))

            return carry

        lax.fori_loop(0, nj, body, 0)

    stage(0)
    strip(0)
    stage(1)
    finish(0, nj - 1, True)
    strip(1)
    finish(1, nj - 1)

    for s in range(2):
        for j in range(nj):
            p_send(s, j).wait_send()

    @pl.when(sends_b)
    def _():
        for c, blk in b_sends:
            x_send(c, blk, (other_pp, blk), (c, blk) == (0, 1)).wait_send()

    @pl.when(keeps_a)
    def _():
        for c in range(len(X_ROWS)):
            x_send(c, 1, (pp, 1)).wait_send()

    @pl.when(on_s0)
    def _():
        for s in range(2):
            for j in range(nj):
                z_send(s, j).wait_send()

    @pl.when(on_s1)
    def _():
        for s in range(2):
            for j in range(nj):
                z_send(s, j).wait_recv()
                weave(s, j, za, 0)


def solution(mesh):
    half = mesh.shape["pp"] // 2

    def local_step(act, w, scale, shift):
        nn, hh, ww, cc = act.shape
        ch = cc // 2
        nj = ch // TILE
        row = ww * nn
        x = act.transpose(1, 2, 0, 3)
        w = w.reshape(9, ch, cc)
        m0, m1 = ((hi - lo) * row for lo, hi in OUT_ROWS)
        anyspec = pl.BlockSpec(memory_space=pl.ANY)
        vspec = pl.BlockSpec(memory_space=pltpu.VMEM)
        dma = pltpu.SemaphoreType.DMA
        npc = len(X_ROWS)
        out = pl.pallas_call(
            functools.partial(conv_kernel, half),
            out_shape=pltpu.VMEM((hh * ww, 2 * nn, ch), jnp.bfloat16),
            in_specs=[anyspec] * 4,
            out_specs=vspec,
            scratch_shapes=[
                pltpu.VMEM((2 * nj, TILE // 2), jnp.float32),
                pltpu.VMEM((2 * nj, TILE // 2), jnp.float32),
                pltpu.VMEM((X_ROWS[0][1], ww, nn, ch), jnp.bfloat16),
                pltpu.VMEM((hh, ww, nn, ch), jnp.bfloat16),
                pltpu.VMEM((6, (hh + 2) * row, ch), jnp.bfloat16),
                pltpu.VMEM((2, 9, ch, 2 * TILE), jnp.bfloat16),
                pltpu.VMEM((nj, m0, TILE), jnp.float32),
                pltpu.VMEM((nj, m1, TILE), jnp.float32),
                pltpu.VMEM((nj, m0, TILE), jnp.float32),
                pltpu.VMEM((nj, m1, TILE), jnp.float32),
                pltpu.VMEM((nj, max(m0, m1), TILE), jnp.float32),
                pltpu.VMEM((nj, hh * row, TILE), jnp.bfloat16),
                pltpu.VMEM((nj, hh * row, TILE), jnp.bfloat16),
                dma((2,)), dma, pltpu.SemaphoreType.REGULAR, dma((npc, 2)), dma((npc,)), dma((npc,)), dma((2, 2)),
                dma((2, nj)), dma((2, nj)), dma((2, nj)), dma((2, nj)),
            ],
            compiler_params=pltpu.CompilerParams(collective_id=0, has_side_effects=True, vmem_limit_bytes=VMEM_LIMIT),
        )(x, w, scale.reshape(2 * nj, TILE // 2), shift.reshape(2 * nj, TILE // 2))
        return out.reshape(hh, ww, 2 * nn, ch).transpose(2, 0, 1, 3)

    return jax.shard_map(local_step, mesh=mesh, in_specs=(P(("pp", "tp")), P(None, None, "tp", None), P("tp"), P("tp")), out_specs=P("pp", None, None, "tp"), check_vma=False)
```

```python
import functools

import jax
import jax.numpy as jnp
from jax import lax
from jax.experimental import pallas as pl
from jax.experimental.pallas import tpu as pltpu
from jax.sharding import PartitionSpec as P

MESH = pl.DeviceIdType.MESH
TILE = 256
X_ROWS = ((0, 2), (2, 8), (8, 14))
STAGED = ((0, 1), (2,))
OUT_ROWS = ((0, 6), (6, 14))
HOLD = 3
VMEM_LIMIT = 62000000


def conv_kernel(half, x, w, scale_in, shift_in, out, scale, shift, first, xr, xs, wbuf, ps0, ps1, pr0, pr1, pown, zbuf, za,
                csem, fsem, late, xsend, xrecv, xloc, wsem, psend, precv, zsend, zrecv):
    pp, tp = lax.axis_index("pp"), lax.axis_index("tp")
    on_s1 = pp >= half
    on_s0 = jnp.logical_not(on_s1)
    other_pp = jnp.where(on_s1, pp - half, pp + half)
    peer = 1 - tp
    sends_b = jnp.logical_and(on_s0, tp == 1)
    keeps_a = jnp.logical_and(on_s0, tp == 0)
    late_core = jnp.logical_and(on_s1, tp == 0)
    hh, ww, nn, cc = x.shape
    ch = cc // 2
    row = ww * nn
    nj = ch // TILE
    hold = HOLD
    ps, pr = (ps0, ps1), (pr0, pr1)

    def w_copies(j, slot):
        for k, blk in enumerate((tp, peer)):
            cols = pl.ds(pl.multiple_of(blk * ch + j * TILE, TILE), TILE)
            yield pltpu.make_async_copy(w.at[:, :, cols], wbuf.at[slot, :, :, pl.ds(k * TILE, TILE)], wsem.at[slot, k])

    def x_send(c, blk, dst, from_vmem=False):
        lo, hi = X_ROWS[c]
        return pltpu.make_async_remote_copy(
            src_ref=first if from_vmem else x.at[pl.ds(lo, hi - lo), :, :, pl.ds(blk * ch, ch)],
            dst_ref=xr.at[pl.ds(lo, hi - lo)],
            send_sem=xsend.at[c, blk], recv_sem=xrecv.at[c],
            device_id=dst, device_id_type=MESH)

    def x_keep(c):
        lo, hi = X_ROWS[c]
        return pltpu.make_async_copy(x.at[pl.ds(lo, hi - lo), :, :, pl.ds(0, ch)], xr.at[pl.ds(lo, hi - lo)], xloc.at[c])

    def p_send(s, j):
        return pltpu.make_async_remote_copy(
            src_ref=ps[s].at[j], dst_ref=pr[s].at[j], send_sem=psend.at[s, j], recv_sem=precv.at[s, j],
            device_id=(pp, peer), device_id_type=MESH)

    def z_rows(s):
        lo, hi = OUT_ROWS[s]
        return pl.ds(lo * row, (hi - lo) * row)

    def z_send(s, j):
        return pltpu.make_async_remote_copy(
            src_ref=zbuf.at[j, z_rows(s)], dst_ref=za.at[j, z_rows(s)], send_sem=zsend.at[s, j], recv_sem=zrecv.at[s, j],
            device_id=(other_pp, tp), device_id_type=MESH)

    def weave(s, j, src, group):
        lo, hi = OUT_ROWS[s]
        cols = pl.ds(pl.multiple_of(j * TILE, TILE), TILE)
        for k in range(lo * ww, hi * ww):
            out[k, pl.ds(group * nn, nn), cols] = src[j, pl.ds(k * nn, nn), :]

    def channel(ref, j):
        return jnp.concatenate([ref[pl.ds(2 * j, 1), :], ref[pl.ds(2 * j + 1, 1), :]], axis=1)

    barrier = pltpu.get_barrier_semaphore()

    @pl.when(on_s1)
    def _():
        pl.semaphore_signal(barrier, inc=1, device_id=(other_pp, tp), device_id_type=MESH)

    pl.semaphore_signal(barrier, inc=1, device_id=(pp, peer), device_id_type=MESH)

    @pl.when(sends_b)
    def _():
        pl.semaphore_signal(barrier, inc=1, device_id=(other_pp, 0), device_id_type=MESH)

    load_first = pltpu.make_async_copy(x.at[pl.ds(0, X_ROWS[0][1]), :, :, pl.ds(ch, ch)], first, fsem)

    @pl.when(sends_b)
    def _():
        load_first.start()

    @pl.when(keeps_a)
    def _():
        for c in range(len(X_ROWS)):
            x_keep(c).start()

    channel_copies = [pltpu.make_async_copy(scale_in, scale, csem.at[0]), pltpu.make_async_copy(shift_in, shift, csem.at[1])]
    for copy in [*w_copies(0, 0), *channel_copies]:
        copy.start()

    @pl.when(sends_b)
    def _():
        load_first.wait()

    pl.semaphore_wait(barrier, jnp.where(jnp.logical_and(on_s1, tp == 1), 1, 2))

    @pl.when(late_core)
    def _():
        pl.semaphore_signal(late, inc=1, device_id=(other_pp, 1), device_id_type=MESH)

    b_sends = [(c, blk) for cs in STAGED for blk in (1, 0) for c in cs]

    @pl.when(sends_b)
    def _():
        for c, blk in b_sends:
            if (c, blk) == (0, 0):
                pl.semaphore_wait(late, 1)
            x_send(c, blk, (other_pp, blk), (c, blk) == (0, 1)).start()

    @pl.when(keeps_a)
    def _():
        for c in range(len(X_ROWS)):
            x_send(c, 1, (pp, 1)).start()

    for copy in channel_copies:
        copy.wait()

    @pl.when(on_s0)
    def _():
        out[...] = jnp.zeros_like(out)

    zrow = jnp.zeros((row, ch), xs.dtype)
    zpos = jnp.zeros((nn, ch), xs.dtype)
    for b in range(3):
        xs[b, pl.ds(0, row), :] = zrow
        xs[b, pl.ds((hh + 1) * row, row), :] = zrow
    for h in range(hh):
        for b, wo in ((0, 0), (2, ww - 1)):
            xs[b, pl.ds((h + 1) * row + wo * nn, nn), :] = zpos
            xs[3 + b, pl.ds(h * row + wo * nn, nn), :] = zpos

    def stage(s):
        lo, hi = X_ROWS[STAGED[s][0]][0], X_ROWS[STAGED[s][-1]][1]

        @pl.when(keeps_a)
        def _():
            for c in STAGED[s]:
                x_keep(c).wait()

        @pl.when(jnp.logical_not(keeps_a))
        def _():
            for c in STAGED[s]:
                x_send(c, 0, (other_pp, 0)).wait_recv()

        def pair(hp, carry):
            base = pl.multiple_of(hp * (2 * row), 2 * row)
            for e in range(2):
                for wi in range(ww):
                    piece = xr[2 * hp + e, wi]
                    for b in range(3):
                        wo = wi + 1 - b
                        if 0 <= wo < ww:
                            off = e * row + wo * nn
                            xs.at[b, pl.ds(base, 3 * row), :][pl.ds(row + off, nn), :] = piece
                            xs.at[3 + b, pl.ds(base, 2 * row), :][pl.ds(off, nn), :] = piece
            return carry

        lax.fori_loop(lo // 2, hi // 2, pair, 0)

    def finish(s, j):
        lo, hi = OUT_ROWS[s]
        m = (hi - lo) * row
        p_send(s, j).wait_recv()
        pre = pown[j, pl.ds(0, m), :] + pr[s][j]
        y = pre * channel(scale, j) + channel(shift, j)
        zbuf[j, z_rows(s), :] = jnp.maximum(y, 0.0).astype(zbuf.dtype)

        @pl.when(on_s1)
        def _():
            weave(s, j, zbuf, 1)

    def step(s, j, has_next):
        lo, hi = OUT_ROWS[s]
        m = (hi - lo) * row
        turn = s * nj + j
        slot = lax.rem(turn, 2)
        for copy in w_copies(j, slot):
            copy.wait()

        @pl.when(has_next)
        def _():
            for copy in w_copies(lax.rem(j + 1, nj), 1 - slot):
                copy.start()

        acc = None
        for a in range(3):
            for b in range(3):
                if a == 1:
                    lhs = xs[3 + b, pl.ds(lo * row, m), :]
                else:
                    lhs = xs[b, pl.ds((lo + a) * row, m), :]
                term = jnp.dot(lhs, wbuf[slot, 3 * a + b], preferred_element_type=jnp.float32)
                acc = term if acc is None else acc + term
        ps[s][j] = acc[:, TILE:]
        pown[j, pl.ds(0, m), :] = acc[:, :TILE]

    def start_z(s, j, when):
        @pl.when(when)
        def _():
            z_send(s, j).start()

    def strip(s):
        def body(j, carry):
            if s == 1:
                @pl.when(jnp.logical_and(keeps_a, j == hold))
                def _():
                    for s2, j2 in [(0, i) for i in range(nj)] + [(1, i) for i in range(hold - 2)]:
                        z_send(s2, j2).start()

            step(s, j, s * nj + j + 1 < 2 * nj)

            free = sends_b if s == 0 else jnp.logical_or(sends_b, jnp.logical_and(keeps_a, j >= hold))
            start_z(s, j - 2, jnp.logical_and(free, j > 1))
            if s == 1:
                start_z(0, nj - 1, jnp.logical_and(sends_b, j == 0))

            @pl.when(j > 0)
            def _():
                finish(s, j - 1)

            p_send(s, j).start()
            return carry

        lax.fori_loop(0, nj, body, 0)

    stage(0)
    strip(0)
    stage(1)
    start_z(0, nj - 2, sends_b)
    finish(0, nj - 1)
    strip(1)
    start_z(1, nj - 2, on_s0)
    finish(1, nj - 1)

    for s in range(2):
        for j in range(nj):
            p_send(s, j).wait_send()

    @pl.when(sends_b)
    def _():
        for c, blk in b_sends:
            x_send(c, blk, (other_pp, blk), (c, blk) == (0, 1)).wait_send()

    @pl.when(keeps_a)
    def _():
        for c in range(len(X_ROWS)):
            x_send(c, 1, (pp, 1)).wait_send()

    @pl.when(on_s0)
    def _():
        z_send(1, nj - 1).start()
        for s in range(2):
            for j in range(nj):
                z_send(s, j).wait_send()

    @pl.when(on_s1)
    def _():
        for s in range(2):
            for j in range(nj):
                z_send(s, j).wait_recv()
                weave(s, j, za, 0)


def solution(mesh):
    half = mesh.shape["pp"] // 2

    def local_step(act, w, scale, shift):
        nn, hh, ww, cc = act.shape
        ch = cc // 2
        nj = ch // TILE
        row = ww * nn
        x = act.transpose(1, 2, 0, 3)
        w = w.reshape(9, ch, cc)
        m0, m1 = ((hi - lo) * row for lo, hi in OUT_ROWS)
        anyspec = pl.BlockSpec(memory_space=pl.ANY)
        vspec = pl.BlockSpec(memory_space=pltpu.VMEM)
        dma = pltpu.SemaphoreType.DMA
        npc = len(X_ROWS)
        out = pl.pallas_call(
            functools.partial(conv_kernel, half),
            out_shape=pltpu.VMEM((hh * ww, 2 * nn, ch), jnp.bfloat16),
            in_specs=[anyspec] * 4,
            out_specs=vspec,
            scratch_shapes=[
                pltpu.VMEM((2 * nj, TILE // 2), jnp.float32),
                pltpu.VMEM((2 * nj, TILE // 2), jnp.float32),
                pltpu.VMEM((X_ROWS[0][1], ww, nn, ch), jnp.bfloat16),
                pltpu.VMEM((hh, ww, nn, ch), jnp.bfloat16),
                pltpu.VMEM((6, (hh + 2) * row, ch), jnp.bfloat16),
                pltpu.VMEM((2, 9, ch, 2 * TILE), jnp.bfloat16),
                pltpu.VMEM((nj, m0, TILE), jnp.float32),
                pltpu.VMEM((nj, m1, TILE), jnp.float32),
                pltpu.VMEM((nj, m0, TILE), jnp.float32),
                pltpu.VMEM((nj, m1, TILE), jnp.float32),
                pltpu.VMEM((nj, max(m0, m1), TILE), jnp.float32),
                pltpu.VMEM((nj, hh * row, TILE), jnp.bfloat16),
                pltpu.VMEM((nj, hh * row, TILE), jnp.bfloat16),
                dma((2,)), dma, pltpu.SemaphoreType.REGULAR, dma((npc, 2)), dma((npc,)), dma((npc,)), dma((2, 2)),
                dma((2, nj)), dma((2, nj)), dma((2, nj)), dma((2, nj)),
            ],
            compiler_params=pltpu.CompilerParams(collective_id=0, has_side_effects=True, vmem_limit_bytes=VMEM_LIMIT),
        )(x, w, scale.reshape(2 * nj, TILE // 2), shift.reshape(2 * nj, TILE // 2))
        return out.reshape(hh, ww, 2 * nn, ch).transpose(2, 0, 1, 3)

    return jax.shard_map(local_step, mesh=mesh, in_specs=(P(("pp", "tp")), P(None, None, "tp", None), P("tp"), P("tp")), out_specs=P("pp", None, None, "tp"), check_vma=False)
```

```python
import functools

import jax
import jax.numpy as jnp
from jax import lax
from jax.experimental import pallas as pl
from jax.experimental.pallas import tpu as pltpu
from jax.sharding import PartitionSpec as P

MESH = pl.DeviceIdType.MESH
TILE = 256
X_ROWS = ((0, 2), (2, 8), (8, 14))
STAGED = ((0, 1), (2,))
OUT_ROWS = ((0, 6), (6, 14))
HOLD = 3
VMEM_LIMIT = 62000000


def conv_kernel(half, x, w, scale_in, shift_in, out, scale, shift, first, xr, xs, wbuf, ps0, ps1, pr0, pr1, pown, zbuf, za,
                csem, fsem, late, xsend, xrecv, xloc, wsem, psend, precv, zsend, zrecv):
    pp, tp = lax.axis_index("pp"), lax.axis_index("tp")
    on_s1 = pp >= half
    on_s0 = jnp.logical_not(on_s1)
    other_pp = jnp.where(on_s1, pp - half, pp + half)
    peer = 1 - tp
    sends_b = jnp.logical_and(on_s0, tp == 1)
    keeps_a = jnp.logical_and(on_s0, tp == 0)
    late_core = jnp.logical_and(on_s1, tp == 0)
    hh, ww, nn, cc = x.shape
    ch = cc // 2
    row = ww * nn
    nj = ch // TILE
    hold = HOLD
    ps, pr = (ps0, ps1), (pr0, pr1)

    def w_copies(j, slot):
        for k, blk in enumerate((tp, peer)):
            cols = pl.ds(pl.multiple_of(blk * ch + j * TILE, TILE), TILE)
            yield pltpu.make_async_copy(w.at[:, :, cols], wbuf.at[slot, :, :, pl.ds(k * TILE, TILE)], wsem.at[slot])

    def x_copy(lo, hi, s, blk, dst, src=None):
        return pltpu.make_async_remote_copy(
            src_ref=x.at[pl.ds(lo, hi - lo), :, :, pl.ds(blk * ch, ch)] if src is None else src,
            dst_ref=xr.at[pl.ds(lo, hi - lo)],
            send_sem=xsend.at[blk], recv_sem=xrecv.at[s],
            device_id=dst, device_id_type=MESH)

    def x_send(c, blk, dst, from_vmem=False):
        s = 0 if c in STAGED[0] else 1
        return x_copy(*X_ROWS[c], s, blk, dst, first if from_vmem else None)

    def staged_rows(s):
        return X_ROWS[STAGED[s][0]][0], X_ROWS[STAGED[s][-1]][1]

    def x_keep(s):
        lo, hi = staged_rows(s)
        return pltpu.make_async_copy(x.at[pl.ds(lo, hi - lo), :, :, pl.ds(0, ch)], xr.at[pl.ds(lo, hi - lo)], xloc.at[s])

    def p_send(s, j):
        return pltpu.make_async_remote_copy(
            src_ref=ps[s].at[j], dst_ref=pr[s].at[j], send_sem=psend.at[s], recv_sem=precv.at[s, j],
            device_id=(pp, peer), device_id_type=MESH)

    def z_rows(s):
        lo, hi = OUT_ROWS[s]
        return pl.ds(lo * row, (hi - lo) * row)

    def z_copy(tiles, rows, group):
        return pltpu.make_async_remote_copy(
            src_ref=zbuf.at[tiles, rows], dst_ref=za.at[tiles, rows], send_sem=zsend, recv_sem=zrecv.at[group],
            device_id=(other_pp, tp), device_id_type=MESH)

    def z_send(s, j):
        return z_copy(j, z_rows(s), s)

    last_lo, last_hi = OUT_ROWS[1]
    last_mid = (last_lo + last_hi) // 2
    halves = ((last_lo, last_mid), (last_mid, last_hi))

    def z_last(i):
        lo, hi = halves[i]
        return z_copy(nj - 1, pl.ds(lo * row, (hi - lo) * row), 2 + i)

    def weave(rows, j, src, group):
        lo, hi = rows
        cols = pl.ds(pl.multiple_of(j * TILE, TILE), TILE)
        for k in range(lo * ww, hi * ww):
            out[k, pl.ds(group * nn, nn), cols] = src[j, pl.ds(k * nn, nn), :]

    def channel(ref, j):
        return jnp.concatenate([ref[pl.ds(2 * j, 1), :], ref[pl.ds(2 * j + 1, 1), :]], axis=1)

    barrier = pltpu.get_barrier_semaphore()

    @pl.when(on_s1)
    def _():
        pl.semaphore_signal(barrier, inc=1, device_id=(other_pp, tp), device_id_type=MESH)

    pl.semaphore_signal(barrier, inc=1, device_id=(pp, peer), device_id_type=MESH)

    @pl.when(sends_b)
    def _():
        pl.semaphore_signal(barrier, inc=1, device_id=(other_pp, 0), device_id_type=MESH)

    load_first = pltpu.make_async_copy(x.at[pl.ds(0, X_ROWS[0][1]), :, :, pl.ds(ch, ch)], first, fsem)

    @pl.when(sends_b)
    def _():
        load_first.start()

    @pl.when(keeps_a)
    def _():
        for s in range(2):
            x_keep(s).start()

    channel_copies = [pltpu.make_async_copy(scale_in, scale, csem.at[0]), pltpu.make_async_copy(shift_in, shift, csem.at[1])]
    for copy in [*w_copies(0, 0), *channel_copies]:
        copy.start()

    @pl.when(sends_b)
    def _():
        load_first.wait()

    pl.semaphore_wait(barrier, jnp.where(jnp.logical_and(on_s1, tp == 1), 1, 2))

    @pl.when(late_core)
    def _():
        pl.semaphore_signal(late, inc=1, device_id=(other_pp, 1), device_id_type=MESH)

    b_sends = [(c, blk) for cs in STAGED for blk in (1, 0) for c in cs]

    @pl.when(sends_b)
    def _():
        for c, blk in b_sends:
            if (c, blk) == (0, 0):
                pl.semaphore_wait(late, 1)
            x_send(c, blk, (other_pp, blk), (c, blk) == (0, 1)).start()

    @pl.when(keeps_a)
    def _():
        for c in range(len(X_ROWS)):
            x_send(c, 1, (pp, 1)).start()

    for copy in channel_copies:
        copy.wait()

    @pl.when(on_s0)
    def _():
        out[...] = jnp.zeros_like(out)

    zrow = jnp.zeros((row, ch), xs.dtype)
    zpos = jnp.zeros((nn, ch), xs.dtype)
    for b in range(3):
        xs[b, pl.ds(0, row), :] = zrow
        xs[b, pl.ds((hh + 1) * row, row), :] = zrow
    for h in range(hh):
        for b, wo in ((0, 0), (2, ww - 1)):
            xs[b, pl.ds((h + 1) * row + wo * nn, nn), :] = zpos
            xs[3 + b, pl.ds(h * row + wo * nn, nn), :] = zpos

    def stage(s):
        lo, hi = staged_rows(s)

        @pl.when(keeps_a)
        def _():
            x_keep(s).wait()

        @pl.when(jnp.logical_not(keeps_a))
        def _():
            x_copy(lo, hi, s, 0, (other_pp, 0)).wait_recv()

        def pair(hp, carry):
            base = pl.multiple_of(hp * (2 * row), 2 * row)
            for e in range(2):
                for wi in range(ww):
                    piece = xr[2 * hp + e, wi]
                    for b in range(3):
                        wo = wi + 1 - b
                        if 0 <= wo < ww:
                            off = e * row + wo * nn
                            xs.at[b, pl.ds(base, 3 * row), :][pl.ds(row + off, nn), :] = piece
                            xs.at[3 + b, pl.ds(base, 2 * row), :][pl.ds(off, nn), :] = piece
            return carry

        lax.fori_loop(lo // 2, hi // 2, pair, 0)

    def finish(s, j):
        lo, hi = OUT_ROWS[s]
        m = (hi - lo) * row
        p_send(s, j).wait_recv()
        pre = pown[j, pl.ds(0, m), :] + pr[s][j]
        y = pre * channel(scale, j) + channel(shift, j)
        zbuf[j, z_rows(s), :] = jnp.maximum(y, 0.0).astype(zbuf.dtype)

        @pl.when(on_s1)
        def _():
            weave(OUT_ROWS[s], j, zbuf, 1)

    def step(s, j, has_next):
        lo, hi = OUT_ROWS[s]
        m = (hi - lo) * row
        turn = s * nj + j
        slot = lax.rem(turn, 2)
        pltpu.make_async_copy(w.at[:, :, pl.ds(0, 2 * TILE)], wbuf.at[slot], wsem.at[slot]).wait()

        @pl.when(has_next)
        def _():
            for copy in w_copies(lax.rem(j + 1, nj), 1 - slot):
                copy.start()

        acc = None
        for a in range(3):
            for b in range(3):
                if a == 1:
                    lhs = xs[3 + b, pl.ds(lo * row, m), :]
                else:
                    lhs = xs[b, pl.ds((lo + a) * row, m), :]
                term = jnp.dot(lhs, wbuf[slot, 3 * a + b], preferred_element_type=jnp.float32)
                acc = term if acc is None else acc + term
        ps[s][j] = acc[:, TILE:]
        pown[j, pl.ds(0, m), :] = acc[:, :TILE]

    def start_z(s, j, when):
        @pl.when(when)
        def _():
            z_send(s, j).start()

    def strip(s):
        def body(j, carry):
            if s == 1:
                @pl.when(jnp.logical_and(keeps_a, j == hold))
                def _():
                    for s2, j2 in [(0, i) for i in range(nj)] + [(1, i) for i in range(hold - 2)]:
                        z_send(s2, j2).start()

            step(s, j, s * nj + j + 1 < 2 * nj)

            free = sends_b if s == 0 else jnp.logical_or(sends_b, jnp.logical_and(keeps_a, j >= hold))
            start_z(s, j - 2, jnp.logical_and(free, j > 1))
            if s == 1:
                start_z(0, nj - 1, jnp.logical_and(sends_b, j == 0))

            @pl.when(j > 0)
            def _():
                finish(s, j - 1)

            p_send(s, j).start()
            return carry

        lax.fori_loop(0, nj, body, 0)

    stage(0)
    strip(0)
    stage(1)
    start_z(0, nj - 2, sends_b)
    finish(0, nj - 1)
    strip(1)
    start_z(1, nj - 2, on_s0)
    finish(1, nj - 1)

    for s in range(2):
        pltpu.make_async_remote_copy(
            src_ref=ps[s], dst_ref=pr[s], send_sem=psend.at[s], recv_sem=precv.at[s, 0],
            device_id=(pp, peer), device_id_type=MESH).wait_send()

    @pl.when(sends_b)
    def _():
        for blk in range(2):
            x_copy(0, hh, 0, blk, (other_pp, blk)).wait_send()

    @pl.when(keeps_a)
    def _():
        x_copy(0, hh, 0, 1, (pp, 1)).wait_send()

    @pl.when(on_s0)
    def _():
        for i in range(2):
            z_last(i).start()
        z_copy(pl.ds(0, nj), pl.ds(0, hh * row), 0).wait_send()

    @pl.when(on_s1)
    def _():
        for s, n in ((0, nj), (1, nj - 1)):
            z_copy(pl.ds(0, n), z_rows(s), s).wait_recv()
            for j in range(n):
                weave(OUT_ROWS[s], j, za, 0)
        for i in range(2):
            z_last(i).wait_recv()
            weave(halves[i], nj - 1, za, 0)


def solution(mesh):
    half = mesh.shape["pp"] // 2

    def local_step(act, w, scale, shift):
        nn, hh, ww, cc = act.shape
        ch = cc // 2
        nj = ch // TILE
        row = ww * nn
        x = act.transpose(1, 2, 0, 3)
        w = w.reshape(9, ch, cc)
        m0, m1 = ((hi - lo) * row for lo, hi in OUT_ROWS)
        anyspec = pl.BlockSpec(memory_space=pl.ANY)
        vspec = pl.BlockSpec(memory_space=pltpu.VMEM)
        dma = pltpu.SemaphoreType.DMA
        out = pl.pallas_call(
            functools.partial(conv_kernel, half),
            out_shape=pltpu.VMEM((hh * ww, 2 * nn, ch), jnp.bfloat16),
            in_specs=[anyspec] * 4,
            out_specs=vspec,
            scratch_shapes=[
                pltpu.VMEM((2 * nj, TILE // 2), jnp.float32),
                pltpu.VMEM((2 * nj, TILE // 2), jnp.float32),
                pltpu.VMEM((X_ROWS[0][1], ww, nn, ch), jnp.bfloat16),
                pltpu.VMEM((hh, ww, nn, ch), jnp.bfloat16),
                pltpu.VMEM((6, (hh + 2) * row, ch), jnp.bfloat16),
                pltpu.VMEM((2, 9, ch, 2 * TILE), jnp.bfloat16),
                pltpu.VMEM((nj, m0, TILE), jnp.float32),
                pltpu.VMEM((nj, m1, TILE), jnp.float32),
                pltpu.VMEM((nj, m0, TILE), jnp.float32),
                pltpu.VMEM((nj, m1, TILE), jnp.float32),
                pltpu.VMEM((nj, max(m0, m1), TILE), jnp.float32),
                pltpu.VMEM((nj, hh * row, TILE), jnp.bfloat16),
                pltpu.VMEM((nj, hh * row, TILE), jnp.bfloat16),
                dma((2,)), dma, pltpu.SemaphoreType.REGULAR, dma((2,)), dma((2,)), dma((2,)), dma((2,)),
                dma((2,)), dma((2, nj)), dma, dma((4,)),
            ],
            compiler_params=pltpu.CompilerParams(collective_id=0, has_side_effects=True, vmem_limit_bytes=VMEM_LIMIT),
        )(x, w, scale.reshape(2 * nj, TILE // 2), shift.reshape(2 * nj, TILE // 2))
        return out.reshape(hh, ww, 2 * nn, ch).transpose(2, 0, 1, 3)

    return jax.shard_map(local_step, mesh=mesh, in_specs=(P(("pp", "tp")), P(None, None, "tp", None), P("tp"), P("tp")), out_specs=P("pp", None, None, "tp"), check_vma=False)
```

```python
import functools

import jax
import jax.numpy as jnp
from jax import lax
from jax.experimental import pallas as pl
from jax.experimental.pallas import tpu as pltpu
from jax.sharding import PartitionSpec as P

MESH = pl.DeviceIdType.MESH
TILE = 256
X_ROWS = ((0, 2), (2, 8), (8, 14))
STAGED = ((0, 1), (2,))
OUT_ROWS = ((0, 6), (6, 14))
HOLD = 3
VMEM_LIMIT = 62000000


def conv_kernel(half, x, w, scale_in, shift_in, out, scale, shift, first, xr, xs, wbuf, ps0, ps1, pr0, pr1, pown, zbuf, za,
                csem, fsem, late, xsend, xrecv, xloc, wsem, psend, precv, zsend, zrecv):
    pp, tp = lax.axis_index("pp"), lax.axis_index("tp")
    on_s1 = pp >= half
    on_s0 = jnp.logical_not(on_s1)
    other_pp = jnp.where(on_s1, pp - half, pp + half)
    peer = 1 - tp
    sends_b = jnp.logical_and(on_s0, tp == 1)
    keeps_a = jnp.logical_and(on_s0, tp == 0)
    late_core = jnp.logical_and(on_s1, tp == 0)
    hh, ww, nn, cc = x.shape
    ch = cc // 2
    row = ww * nn
    nj = ch // TILE
    hold = HOLD
    ps, pr = (ps0, ps1), (pr0, pr1)

    def w_copies(j, slot):
        for k, blk in enumerate((tp, peer)):
            cols = pl.ds(pl.multiple_of(blk * ch + j * TILE, TILE), TILE)
            yield pltpu.make_async_copy(w.at[:, :, cols], wbuf.at[slot, :, :, pl.ds(k * TILE, TILE)], wsem.at[slot])

    def x_copy(lo, hi, s, blk, dst, src=None):
        return pltpu.make_async_remote_copy(
            src_ref=x.at[pl.ds(lo, hi - lo), :, :, pl.ds(blk * ch, ch)] if src is None else src,
            dst_ref=xr.at[pl.ds(lo, hi - lo)],
            send_sem=xsend.at[blk], recv_sem=xrecv.at[s],
            device_id=dst, device_id_type=MESH)

    def x_send(c, blk, dst, from_vmem=False):
        s = 0 if c in STAGED[0] else 1
        return x_copy(*X_ROWS[c], s, blk, dst, first if from_vmem else None)

    def staged_rows(s):
        return X_ROWS[STAGED[s][0]][0], X_ROWS[STAGED[s][-1]][1]

    def x_keep(s):
        lo, hi = staged_rows(s)
        return pltpu.make_async_copy(x.at[pl.ds(lo, hi - lo), :, :, pl.ds(0, ch)], xr.at[pl.ds(lo, hi - lo)], xloc.at[s])

    def p_send(s, j):
        return pltpu.make_async_remote_copy(
            src_ref=ps[s].at[j], dst_ref=pr[s].at[j], send_sem=psend.at[s], recv_sem=precv.at[s, j],
            device_id=(pp, peer), device_id_type=MESH)

    def z_rows(s):
        lo, hi = OUT_ROWS[s]
        return pl.ds(lo * row, (hi - lo) * row)

    def z_copy(tiles, rows, group):
        return pltpu.make_async_remote_copy(
            src_ref=zbuf.at[tiles, rows], dst_ref=za.at[tiles, rows], send_sem=zsend, recv_sem=zrecv.at[group],
            device_id=(other_pp, tp), device_id_type=MESH)

    def z_send(s, j):
        return z_copy(j, z_rows(s), s)

    last_lo, last_hi = OUT_ROWS[1]
    last_mid = last_hi - 2
    halves = ((last_lo, last_mid), (last_mid, last_hi))

    def z_last(i):
        lo, hi = halves[i]
        return z_copy(nj - 1, pl.ds(lo * row, (hi - lo) * row), 2 + i)

    def weave(rows, j, src, group):
        lo, hi = rows
        cols = pl.ds(pl.multiple_of(j * TILE, TILE), TILE)
        for k in range(lo * ww, hi * ww):
            out[k, pl.ds(group * nn, nn), cols] = src[j, pl.ds(k * nn, nn), :]

    def channel(ref, j):
        return jnp.concatenate([ref[pl.ds(2 * j, 1), :], ref[pl.ds(2 * j + 1, 1), :]], axis=1)

    barrier = pltpu.get_barrier_semaphore()

    @pl.when(on_s1)
    def _():
        pl.semaphore_signal(barrier, inc=1, device_id=(other_pp, tp), device_id_type=MESH)

    pl.semaphore_signal(barrier, inc=1, device_id=(pp, peer), device_id_type=MESH)

    @pl.when(sends_b)
    def _():
        pl.semaphore_signal(barrier, inc=1, device_id=(other_pp, 0), device_id_type=MESH)

    load_first = pltpu.make_async_copy(x.at[pl.ds(0, X_ROWS[0][1]), :, :, pl.ds(ch, ch)], first, fsem)

    @pl.when(sends_b)
    def _():
        load_first.start()

    @pl.when(keeps_a)
    def _():
        for s in range(2):
            x_keep(s).start()

    channel_copies = [pltpu.make_async_copy(scale_in, scale, csem.at[0]), pltpu.make_async_copy(shift_in, shift, csem.at[1])]
    for copy in [*w_copies(0, 0), *channel_copies]:
        copy.start()

    @pl.when(sends_b)
    def _():
        load_first.wait()

    pl.semaphore_wait(barrier, jnp.where(jnp.logical_and(on_s1, tp == 1), 1, 2))

    @pl.when(late_core)
    def _():
        pl.semaphore_signal(late, inc=1, device_id=(other_pp, 1), device_id_type=MESH)

    b_sends = [(c, blk) for cs in STAGED for blk in (1, 0) for c in cs]

    @pl.when(sends_b)
    def _():
        for c, blk in b_sends:
            if (c, blk) == (0, 0):
                pl.semaphore_wait(late, 1)
            x_send(c, blk, (other_pp, blk), (c, blk) == (0, 1)).start()

    @pl.when(keeps_a)
    def _():
        for c in range(len(X_ROWS)):
            x_send(c, 1, (pp, 1)).start()

    for copy in channel_copies:
        copy.wait()

    @pl.when(on_s0)
    def _():
        out[...] = jnp.zeros_like(out)

    zrow = jnp.zeros((row, ch), xs.dtype)
    zpos = jnp.zeros((nn, ch), xs.dtype)
    for b in range(3):
        xs[b, pl.ds(0, row), :] = zrow
        xs[b, pl.ds((hh + 1) * row, row), :] = zrow
    for h in range(hh):
        for b, wo in ((0, 0), (2, ww - 1)):
            xs[b, pl.ds((h + 1) * row + wo * nn, nn), :] = zpos
            xs[3 + b, pl.ds(h * row + wo * nn, nn), :] = zpos

    def stage(s):
        lo, hi = staged_rows(s)

        @pl.when(keeps_a)
        def _():
            x_keep(s).wait()

        @pl.when(jnp.logical_not(keeps_a))
        def _():
            x_copy(lo, hi, s, 0, (other_pp, 0)).wait_recv()

        def pair(hp, carry):
            base = pl.multiple_of(hp * (2 * row), 2 * row)
            for e in range(2):
                for wi in range(ww):
                    piece = xr[2 * hp + e, wi]
                    for b in range(3):
                        wo = wi + 1 - b
                        if 0 <= wo < ww:
                            off = e * row + wo * nn
                            xs.at[b, pl.ds(base, 3 * row), :][pl.ds(row + off, nn), :] = piece
                            xs.at[3 + b, pl.ds(base, 2 * row), :][pl.ds(off, nn), :] = piece
            return carry

        lax.fori_loop(lo // 2, hi // 2, pair, 0)

    def finish(s, j):
        lo, hi = OUT_ROWS[s]
        m = (hi - lo) * row
        p_send(s, j).wait_recv()
        pre = pown[j, pl.ds(0, m), :] + pr[s][j]
        y = pre * channel(scale, j) + channel(shift, j)
        zbuf[j, z_rows(s), :] = jnp.maximum(y, 0.0).astype(zbuf.dtype)

        @pl.when(on_s1)
        def _():
            weave(OUT_ROWS[s], j, zbuf, 1)

    def step(s, j, has_next):
        lo, hi = OUT_ROWS[s]
        m = (hi - lo) * row
        turn = s * nj + j
        slot = lax.rem(turn, 2)
        pltpu.make_async_copy(w.at[:, :, pl.ds(0, 2 * TILE)], wbuf.at[slot], wsem.at[slot]).wait()

        @pl.when(has_next)
        def _():
            for copy in w_copies(lax.rem(j + 1, nj), 1 - slot):
                copy.start()

        acc = None
        for a in range(3):
            for b in range(3):
                if a == 1:
                    lhs = xs[3 + b, pl.ds(lo * row, m), :]
                else:
                    lhs = xs[b, pl.ds((lo + a) * row, m), :]
                term = jnp.dot(lhs, wbuf[slot, 3 * a + b], preferred_element_type=jnp.float32)
                acc = term if acc is None else acc + term
        ps[s][j] = acc[:, TILE:]
        pown[j, pl.ds(0, m), :] = acc[:, :TILE]

    def start_z(s, j, when):
        @pl.when(when)
        def _():
            z_send(s, j).start()

    def strip(s):
        def body(j, carry):
            if s == 1:
                @pl.when(jnp.logical_and(keeps_a, j == hold))
                def _():
                    for s2, j2 in [(0, i) for i in range(nj)] + [(1, i) for i in range(hold - 2)]:
                        z_send(s2, j2).start()

            step(s, j, s * nj + j + 1 < 2 * nj)

            free = sends_b if s == 0 else jnp.logical_or(sends_b, jnp.logical_and(keeps_a, j >= hold))
            start_z(s, j - 2, jnp.logical_and(free, j > 1))
            if s == 1:
                start_z(0, nj - 1, jnp.logical_and(sends_b, j == 0))

            @pl.when(j > 0)
            def _():
                finish(s, j - 1)

            p_send(s, j).start()
            return carry

        lax.fori_loop(0, nj, body, 0)

    stage(0)
    strip(0)
    stage(1)
    start_z(0, nj - 2, sends_b)
    finish(0, nj - 1)
    strip(1)
    start_z(1, nj - 2, on_s0)
    finish(1, nj - 1)

    for s in range(2):
        pltpu.make_async_remote_copy(
            src_ref=ps[s], dst_ref=pr[s], send_sem=psend.at[s], recv_sem=precv.at[s, 0],
            device_id=(pp, peer), device_id_type=MESH).wait_send()

    @pl.when(sends_b)
    def _():
        for blk in range(2):
            x_copy(0, hh, 0, blk, (other_pp, blk)).wait_send()

    @pl.when(keeps_a)
    def _():
        x_copy(0, hh, 0, 1, (pp, 1)).wait_send()

    @pl.when(on_s0)
    def _():
        for i in range(2):
            z_last(i).start()
        z_copy(pl.ds(0, nj), pl.ds(0, hh * row), 0).wait_send()

    @pl.when(on_s1)
    def _():
        for s, n in ((0, nj), (1, nj - 1)):
            z_copy(pl.ds(0, n), z_rows(s), s).wait_recv()
            for j in range(n):
                weave(OUT_ROWS[s], j, za, 0)
        for i in range(2):
            z_last(i).wait_recv()
            weave(halves[i], nj - 1, za, 0)


def solution(mesh):
    half = mesh.shape["pp"] // 2

    def local_step(act, w, scale, shift):
        nn, hh, ww, cc = act.shape
        ch = cc // 2
        nj = ch // TILE
        row = ww * nn
        x = act.transpose(1, 2, 0, 3)
        w = w.reshape(9, ch, cc)
        m0, m1 = ((hi - lo) * row for lo, hi in OUT_ROWS)
        anyspec = pl.BlockSpec(memory_space=pl.ANY)
        vspec = pl.BlockSpec(memory_space=pltpu.VMEM)
        dma = pltpu.SemaphoreType.DMA
        out = pl.pallas_call(
            functools.partial(conv_kernel, half),
            out_shape=pltpu.VMEM((hh * ww, 2 * nn, ch), jnp.bfloat16),
            in_specs=[anyspec] * 4,
            out_specs=vspec,
            scratch_shapes=[
                pltpu.VMEM((2 * nj, TILE // 2), jnp.float32),
                pltpu.VMEM((2 * nj, TILE // 2), jnp.float32),
                pltpu.VMEM((X_ROWS[0][1], ww, nn, ch), jnp.bfloat16),
                pltpu.VMEM((hh, ww, nn, ch), jnp.bfloat16),
                pltpu.VMEM((6, (hh + 2) * row, ch), jnp.bfloat16),
                pltpu.VMEM((2, 9, ch, 2 * TILE), jnp.bfloat16),
                pltpu.VMEM((nj, m0, TILE), jnp.float32),
                pltpu.VMEM((nj, m1, TILE), jnp.float32),
                pltpu.VMEM((nj, m0, TILE), jnp.float32),
                pltpu.VMEM((nj, m1, TILE), jnp.float32),
                pltpu.VMEM((nj, max(m0, m1), TILE), jnp.float32),
                pltpu.VMEM((nj, hh * row, TILE), jnp.bfloat16),
                pltpu.VMEM((nj, hh * row, TILE), jnp.bfloat16),
                dma((2,)), dma, pltpu.SemaphoreType.REGULAR, dma((2,)), dma((2,)), dma((2,)), dma((2,)),
                dma((2,)), dma((2, nj)), dma, dma((4,)),
            ],
            compiler_params=pltpu.CompilerParams(collective_id=0, has_side_effects=True, vmem_limit_bytes=VMEM_LIMIT),
        )(x, w, scale.reshape(2 * nj, TILE // 2), shift.reshape(2 * nj, TILE // 2))
        return out.reshape(hh, ww, 2 * nn, ch).transpose(2, 0, 1, 3)

    return jax.shard_map(local_step, mesh=mesh, in_specs=(P(("pp", "tp")), P(None, None, "tp", None), P("tp"), P("tp")), out_specs=P("pp", None, None, "tp"), check_vma=False)
```

```python
import functools

import jax
import jax.numpy as jnp
from jax import lax
from jax.experimental import pallas as pl
from jax.experimental.pallas import tpu as pltpu
from jax.sharding import PartitionSpec as P

MESH = pl.DeviceIdType.MESH
TILE = 256
X_ROWS = ((0, 2), (2, 8), (8, 14))
STAGED = ((0, 1), (2,))
OUT_ROWS = ((0, 6), (6, 14))
HOLD = 3
VMEM_LIMIT = 62000000


def conv_kernel(half, x, w, scale_in, shift_in, out, scale, shift, first, xr, xs, wbuf, ps0, ps1, pr0, pr1, pown, zbuf, za,
                csem, fsem, late, xsend, xrecv, xloc, wsem, psend, precv, zsend, zrecv):
    pp, tp = lax.axis_index("pp"), lax.axis_index("tp")
    on_s1 = pp >= half
    on_s0 = jnp.logical_not(on_s1)
    other_pp = jnp.where(on_s1, pp - half, pp + half)
    peer = 1 - tp
    sends_b = jnp.logical_and(on_s0, tp == 1)
    keeps_a = jnp.logical_and(on_s0, tp == 0)
    late_core = jnp.logical_and(on_s1, tp == 0)
    hh, ww, nn, cc = x.shape
    ch = cc // 2
    row = ww * nn
    nj = ch // TILE
    hold = HOLD
    ps, pr = (ps0, ps1), (pr0, pr1)

    def w_copies(j, slot):
        for k, blk in enumerate((tp, peer)):
            cols = pl.ds(pl.multiple_of(blk * ch + j * TILE, TILE), TILE)
            yield pltpu.make_async_copy(w.at[:, :, cols], wbuf.at[slot, :, :, pl.ds(k * TILE, TILE)], wsem.at[slot])

    def x_copy(lo, hi, s, blk, dst, src=None):
        return pltpu.make_async_remote_copy(
            src_ref=x.at[pl.ds(lo, hi - lo), :, :, pl.ds(blk * ch, ch)] if src is None else src,
            dst_ref=xr.at[pl.ds(lo, hi - lo)],
            send_sem=xsend.at[blk], recv_sem=xrecv.at[s],
            device_id=dst, device_id_type=MESH)

    def x_send(c, blk, dst, from_vmem=False):
        s = 0 if c in STAGED[0] else 1
        return x_copy(*X_ROWS[c], s, blk, dst, first if from_vmem else None)

    def staged_rows(s):
        return X_ROWS[STAGED[s][0]][0], X_ROWS[STAGED[s][-1]][1]

    def x_keep(s):
        lo, hi = staged_rows(s)
        return pltpu.make_async_copy(x.at[pl.ds(lo, hi - lo), :, :, pl.ds(0, ch)], xr.at[pl.ds(lo, hi - lo)], xloc.at[s])

    def p_send(s, j):
        return pltpu.make_async_remote_copy(
            src_ref=ps[s].at[j], dst_ref=pr[s].at[j], send_sem=psend.at[s], recv_sem=precv.at[lax.rem(s * nj + j, 2)],
            device_id=(pp, peer), device_id_type=MESH)

    def z_rows(s):
        lo, hi = OUT_ROWS[s]
        return pl.ds(lo * row, (hi - lo) * row)

    def z_copy(tiles, rows, group):
        return pltpu.make_async_remote_copy(
            src_ref=zbuf.at[tiles, rows], dst_ref=za.at[tiles, rows], send_sem=zsend, recv_sem=zrecv.at[group],
            device_id=(other_pp, tp), device_id_type=MESH)

    def z_send(s, j):
        return z_copy(j, z_rows(s), s)

    last_lo, last_hi = OUT_ROWS[1]
    last_mid = last_hi - 2
    halves = ((last_lo, last_mid), (last_mid, last_hi))

    def z_last(i):
        lo, hi = halves[i]
        return z_copy(nj - 1, pl.ds(lo * row, (hi - lo) * row), 2 + i)

    def weave(rows, j, src, group):
        lo, hi = rows
        cols = pl.ds(pl.multiple_of(j * TILE, TILE), TILE)
        for k in range(lo * ww, hi * ww):
            out[k, pl.ds(group * nn, nn), cols] = src[j, pl.ds(k * nn, nn), :]

    def channel(ref, j):
        return jnp.concatenate([ref[pl.ds(2 * j, 1), :], ref[pl.ds(2 * j + 1, 1), :]], axis=1)

    barrier = pltpu.get_barrier_semaphore()

    @pl.when(on_s1)
    def _():
        pl.semaphore_signal(barrier, inc=1, device_id=(other_pp, tp), device_id_type=MESH)

    pl.semaphore_signal(barrier, inc=1, device_id=(pp, peer), device_id_type=MESH)

    @pl.when(sends_b)
    def _():
        pl.semaphore_signal(barrier, inc=1, device_id=(other_pp, 0), device_id_type=MESH)

    load_first = pltpu.make_async_copy(x.at[pl.ds(0, X_ROWS[0][1]), :, :, pl.ds(ch, ch)], first, fsem)

    @pl.when(sends_b)
    def _():
        load_first.start()

    @pl.when(keeps_a)
    def _():
        for s in range(2):
            x_keep(s).start()

    channel_copies = [pltpu.make_async_copy(scale_in, scale, csem.at[0]), pltpu.make_async_copy(shift_in, shift, csem.at[1])]
    for copy in [*w_copies(0, 0), *channel_copies]:
        copy.start()

    @pl.when(sends_b)
    def _():
        load_first.wait()

    pl.semaphore_wait(barrier, jnp.where(jnp.logical_and(on_s1, tp == 1), 1, 2))

    @pl.when(late_core)
    def _():
        pl.semaphore_signal(late, inc=1, device_id=(other_pp, 1), device_id_type=MESH)

    b_sends = [(c, blk) for cs in STAGED for blk in (1, 0) for c in cs]

    @pl.when(sends_b)
    def _():
        for c, blk in b_sends:
            if (c, blk) == (0, 0):
                pl.semaphore_wait(late, 1)
            x_send(c, blk, (other_pp, blk), (c, blk) == (0, 1)).start()

    @pl.when(keeps_a)
    def _():
        for c in range(len(X_ROWS)):
            x_send(c, 1, (pp, 1)).start()

    for copy in channel_copies:
        copy.wait()

    @pl.when(on_s0)
    def _():
        out[...] = jnp.zeros_like(out)

    zrow = jnp.zeros((row, ch), xs.dtype)
    zpos = jnp.zeros((nn, ch), xs.dtype)
    for b in range(3):
        xs[b, pl.ds(0, row), :] = zrow
        xs[b, pl.ds((hh + 1) * row, row), :] = zrow
    for h in range(hh):
        for b, wo in ((0, 0), (2, ww - 1)):
            xs[b, pl.ds((h + 1) * row + wo * nn, nn), :] = zpos
            xs[3 + b, pl.ds(h * row + wo * nn, nn), :] = zpos

    def stage(s):
        lo, hi = staged_rows(s)

        @pl.when(keeps_a)
        def _():
            x_keep(s).wait()

        @pl.when(jnp.logical_not(keeps_a))
        def _():
            x_copy(lo, hi, s, 0, (other_pp, 0)).wait_recv()

        def pair(hp, carry):
            base = pl.multiple_of(hp * (2 * row), 2 * row)
            for e in range(2):
                for wi in range(ww):
                    piece = xr[2 * hp + e, wi]
                    for b in range(3):
                        wo = wi + 1 - b
                        if 0 <= wo < ww:
                            off = e * row + wo * nn
                            xs.at[b, pl.ds(base, 3 * row), :][pl.ds(row + off, nn), :] = piece
                            xs.at[3 + b, pl.ds(base, 2 * row), :][pl.ds(off, nn), :] = piece
            return carry

        lax.fori_loop(lo // 2, hi // 2, pair, 0)

    def finish(s, j):
        lo, hi = OUT_ROWS[s]
        m = (hi - lo) * row
        p_send(s, j).wait_recv()
        pre = pown[j, pl.ds(0, m), :] + pr[s][j]
        y = pre * channel(scale, j) + channel(shift, j)
        zbuf[j, z_rows(s), :] = jnp.maximum(y, 0.0).astype(zbuf.dtype)

        @pl.when(on_s1)
        def _():
            weave(OUT_ROWS[s], j, zbuf, 1)

    def step(s, j, has_next):
        lo, hi = OUT_ROWS[s]
        m = (hi - lo) * row
        turn = s * nj + j
        slot = lax.rem(turn, 2)
        pltpu.make_async_copy(w.at[:, :, pl.ds(0, 2 * TILE)], wbuf.at[slot], wsem.at[slot]).wait()

        @pl.when(has_next)
        def _():
            for copy in w_copies(lax.rem(j + 1, nj), 1 - slot):
                copy.start()

        acc = None
        for a in range(3):
            for b in range(3):
                if a == 1:
                    lhs = xs[3 + b, pl.ds(lo * row, m), :]
                else:
                    lhs = xs[b, pl.ds((lo + a) * row, m), :]
                term = jnp.dot(lhs, wbuf[slot, 3 * a + b], preferred_element_type=jnp.float32)
                acc = term if acc is None else acc + term
        ps[s][j] = acc[:, TILE:]
        pown[j, pl.ds(0, m), :] = acc[:, :TILE]

    def start_z(s, j, when):
        @pl.when(when)
        def _():
            z_send(s, j).start()

    def strip(s):
        def body(j, carry):
            if s == 1:
                @pl.when(jnp.logical_and(keeps_a, j == hold))
                def _():
                    for s2, j2 in [(0, i) for i in range(nj)] + [(1, i) for i in range(hold - 2)]:
                        z_send(s2, j2).start()

            step(s, j, s * nj + j + 1 < 2 * nj)

            free = sends_b if s == 0 else jnp.logical_or(sends_b, jnp.logical_and(keeps_a, j >= hold))
            start_z(s, j - 2, jnp.logical_and(free, j > 1))
            if s == 1:
                start_z(0, nj - 1, jnp.logical_and(sends_b, j == 0))

            @pl.when(j > 0)
            def _():
                finish(s, j - 1)

            p_send(s, j).start()
            return carry

        lax.fori_loop(0, nj, body, 0)

    stage(0)
    strip(0)
    stage(1)
    start_z(0, nj - 2, sends_b)
    finish(0, nj - 1)
    strip(1)
    start_z(1, nj - 2, on_s0)
    finish(1, nj - 1)

    for s in range(2):
        pltpu.make_async_remote_copy(
            src_ref=ps[s], dst_ref=pr[s], send_sem=psend.at[s], recv_sem=precv.at[0],
            device_id=(pp, peer), device_id_type=MESH).wait_send()

    @pl.when(sends_b)
    def _():
        for blk in range(2):
            x_copy(0, hh, 0, blk, (other_pp, blk)).wait_send()

    @pl.when(keeps_a)
    def _():
        x_copy(0, hh, 0, 1, (pp, 1)).wait_send()

    @pl.when(on_s0)
    def _():
        for i in range(2):
            z_last(i).start()
        z_copy(pl.ds(0, nj), pl.ds(0, hh * row), 0).wait_send()

    @pl.when(on_s1)
    def _():
        for s, n in ((0, nj), (1, nj - 1)):
            z_copy(pl.ds(0, n), z_rows(s), s).wait_recv()
            for j in range(n):
                weave(OUT_ROWS[s], j, za, 0)
        for i in range(2):
            z_last(i).wait_recv()
            weave(halves[i], nj - 1, za, 0)


def solution(mesh):
    half = mesh.shape["pp"] // 2

    def local_step(act, w, scale, shift):
        nn, hh, ww, cc = act.shape
        ch = cc // 2
        nj = ch // TILE
        row = ww * nn
        x = act.transpose(1, 2, 0, 3)
        w = w.reshape(9, ch, cc)
        m0, m1 = ((hi - lo) * row for lo, hi in OUT_ROWS)
        anyspec = pl.BlockSpec(memory_space=pl.ANY)
        vspec = pl.BlockSpec(memory_space=pltpu.VMEM)
        dma = pltpu.SemaphoreType.DMA
        out = pl.pallas_call(
            functools.partial(conv_kernel, half),
            out_shape=pltpu.VMEM((hh * ww, 2 * nn, ch), jnp.bfloat16),
            in_specs=[anyspec] * 4,
            out_specs=vspec,
            scratch_shapes=[
                pltpu.VMEM((2 * nj, TILE // 2), jnp.float32),
                pltpu.VMEM((2 * nj, TILE // 2), jnp.float32),
                pltpu.VMEM((X_ROWS[0][1], ww, nn, ch), jnp.bfloat16),
                pltpu.VMEM((hh, ww, nn, ch), jnp.bfloat16),
                pltpu.VMEM((6, (hh + 2) * row, ch), jnp.bfloat16),
                pltpu.VMEM((2, 9, ch, 2 * TILE), jnp.bfloat16),
                pltpu.VMEM((nj, m0, TILE), jnp.float32),
                pltpu.VMEM((nj, m1, TILE), jnp.float32),
                pltpu.VMEM((nj, m0, TILE), jnp.float32),
                pltpu.VMEM((nj, m1, TILE), jnp.float32),
                pltpu.VMEM((nj, max(m0, m1), TILE), jnp.float32),
                pltpu.VMEM((nj, hh * row, TILE), jnp.bfloat16),
                pltpu.VMEM((nj, hh * row, TILE), jnp.bfloat16),
                dma((2,)), dma, pltpu.SemaphoreType.REGULAR, dma((2,)), dma((2,)), dma((2,)), dma((2,)),
                dma((2,)), dma((2,)), dma, dma((4,)),
            ],
            compiler_params=pltpu.CompilerParams(collective_id=0, has_side_effects=True, vmem_limit_bytes=VMEM_LIMIT),
        )(x, w, scale.reshape(2 * nj, TILE // 2), shift.reshape(2 * nj, TILE // 2))
        return out.reshape(hh, ww, 2 * nn, ch).transpose(2, 0, 1, 3)

    return jax.shard_map(local_step, mesh=mesh, in_specs=(P(("pp", "tp")), P(None, None, "tp", None), P("tp"), P("tp")), out_specs=P("pp", None, None, "tp"), check_vma=False)
```
